128 devices in a mesh: gx: 8 (over y, core), gy: 16 (over z, x).
Axes of the slice: x: 4, y: 4, z: 4, core: 2. Of those that a mesh axis runs over, the one named last changes fastest.
Arguments:
- transfer: bfloat16 [2048, 75, 128], P(('gx', 'gy')), may hold values from -6 to 6
- positions: float32 [2048, 3, 128], P(('gx', 'gy')), may hold values from -4 to 4
- normals: float32 [2048, 3, 128], P(('gx', 'gy')), may hold values from -4 to 4
- area: float32 [2048, 128], P(('gx', 'gy')), may hold values from 0.06 to 3
- albedo: float32 [2048, 3, 128], P(('gx', 'gy')), may hold values from 0.3 to 0.9
- pairs: int32 [2048, 40], P(('gx', 'gy')), may hold values from 0 to 2047, as said below
- home: int32 [2048], replicated, may hold values from 0 to 2047, as said below
Outputs:
- bounce_one: bfloat16 [2048, 75, 128], P(('gx', 'gy'))
- bounce_two: bfloat16 [2048, 75, 128], P(('gx', 'gy'))
- energies: float32 [2], replicated
The draws below stay inside these ranges and needn't reach their ends.
Inputs may be any that keep to these rules, and one draw needn't show every extreme that they name: `home`: A permutation; the block in slot s is held by device s // 16, devices counted gx major. `pairs`: the first 16 entries of a row name blocks held by the same device as the row's slot, the other 24 name blocks held by other devices. Over the rows of one device, the far entries name at most 2 distinct blocks of any one other device, and exactly 2 of some. Ids may repeat within a row; each entry counts.
All inputs are finite; a program needn't handle non-finite values.
Results may differ from the reference program's by a relative error of at most 0.02.
Values may be sent and summed in bfloat16 or wider, within the bound.
A program may use at most 128 MiB of HBM per device.

```python
import jax
import jax.numpy as jnp
from jax import lax

BLK_DEV = 16
VERT = 128
COLORS = 3
NEAR = 16
FAR = 24
CAP = 2
CH = 75
BLOCKS = 2048


def layout_tables(key):
    devices_all = BLOCKS // BLK_DEV
    home = jax.random.permutation(jax.random.fold_in(key, 11), BLOCKS).astype(jnp.int32)
    inverse = jnp.argsort(home, stable=True).astype(jnp.int32)
    keys = jax.random.split(jax.random.fold_in(key, 12), 4)
    slot_all = jnp.arange(BLOCKS, dtype=jnp.int32)
    device_of = slot_all // BLK_DEV
    near_local = jax.random.randint(keys[0], (BLOCKS, NEAR), 0, BLK_DEV, dtype=jnp.int32)
    near_slot = device_of[:, None] * BLK_DEV + near_local
    offset = jax.random.randint(keys[1], (BLOCKS, FAR), 1, devices_all, dtype=jnp.int32)
    column = jnp.arange(FAR, dtype=jnp.int32)[None, :]
    forced = (slot_all % BLK_DEV == 0)[:, None] & (column < CAP)
    offset = jnp.where(forced, 1, offset)
    pick_k = jax.random.randint(keys[2], (BLOCKS, FAR), 0, CAP, dtype=jnp.int32)
    pick_k = jnp.where(forced, column, pick_k)
    owner_dev = (device_of[:, None] + offset) % devices_all
    start_tab = jax.random.randint(keys[3], (devices_all, devices_all), 0, BLK_DEV, dtype=jnp.int32)
    local_idx = (start_tab[device_of[:, None], owner_dev] + pick_k) % BLK_DEV
    far_slot = owner_dev * BLK_DEV + local_idx
    source_slot = jnp.concatenate([near_slot, far_slot], axis=1)
    pairs = jnp.take(inverse, source_slot, axis=0).astype(jnp.int32)
    return (home, pairs)


def draw_home(key, part):
    return layout_tables(key)[0]


def draw_pairs(key, part):
    return layout_tables(key)[1]


def draw_area(key, part):
    ramp = jnp.arange(BLOCKS, dtype=jnp.float32)[:, None] / (BLOCKS - 1)
    logs = jax.random.uniform(key, (BLOCKS, VERT), jnp.float32, jnp.log(0.2), jnp.log(2.0))
    return jnp.exp(logs) * (0.5 + ramp)


def shard_levels(own_key, extent, cuts, least, largest):
    gain, own = 1.0, jax.random.fold_in(own_key, 6)
    for position, blocks in cuts:
        draws = jnp.exp(jax.random.uniform(jax.random.fold_in(own, position), (blocks,), jnp.float32, least / len(cuts), largest / len(cuts)))
        gain = gain * jnp.repeat(draws, extent[position] // blocks).reshape([-1 if axis == position else 1 for axis in range(len(extent))])
    return gain


def bell_draw(stream_key, extent, spread, bound, cuts=(), kind=jnp.bfloat16):
    values = spread * jax.random.normal(stream_key, extent, jnp.float32)
    if cuts:
        values = values * shard_levels(stream_key, extent, cuts, -0.22, 0.18)
    return jnp.clip(values, -bound, bound).astype(kind)


def setup_inputs(seed: int = 0) -> dict:
    key_list = jax.random.split(jax.random.key(seed), 8)
    return {
        "transfer": bell_draw(key_list[0], (BLOCKS, CH, VERT), 1.0, 6.0, ((0, 128),)),
        "positions": bell_draw(key_list[1], (BLOCKS, 3, VERT), 1.0, 4.0, ((0, 128),), jnp.float32),
        "normals": bell_draw(key_list[2], (BLOCKS, 3, VERT), 1.0, 4.0, ((0, 128),), jnp.float32),
        "area": draw_area(jax.random.fold_in(key_list[7], 71), 0),
        "albedo": jnp.clip(0.3 + 0.59999996 * jax.random.uniform(key_list[4], (BLOCKS, COLORS, VERT), jnp.float32) ** shard_levels(key_list[4], (BLOCKS, COLORS, VERT), ((0, 128),), -0.2, 0.2), 0.3, 0.9),
        "pairs": draw_pairs(jax.random.fold_in(key_list[7], 71), 0),
        "home": draw_home(jax.random.fold_in(key_list[7], 71), 0),
    }


batch_blocks = 4


def form_tiles(recv_pos, recv_nrm, src_pos, src_nrm, src_area):
    distance = None
    along_p = None
    along_q = None
    for axis_id in range(3):
        gap_vec = src_pos[:, :, axis_id, None, :] - recv_pos[:, None, axis_id, :, None]
        near_term = recv_nrm[:, None, axis_id, :, None] * gap_vec
        far_term = src_nrm[:, :, axis_id, None, :] * gap_vec
        if distance is None:
            distance = gap_vec * gap_vec
            along_p = near_term
            along_q = far_term
        else:
            distance = distance + gap_vec * gap_vec
            along_p = along_p + near_term
            along_q = along_q + far_term
    soft_sq = distance + 1.0
    transfer_factors = jnp.maximum(along_p, 0.0) * jnp.maximum(-along_q, 0.0) * src_area[:, :, None, :] / (jnp.pi * soft_sq * soft_sq)
    return transfer_factors.astype(jnp.bfloat16)


def reflect_all(source_rows, src_positions, src_normals, src_area, pair_row_list, recv_positions, recv_normals):
    turns = pair_row_list.shape[0] // batch_blocks

    def group_term(group_id):
        first_row = group_id * batch_blocks
        picked_rows = lax.dynamic_slice_in_dim(pair_row_list, first_row, batch_blocks, 0)
        recv_pos = lax.dynamic_slice_in_dim(recv_positions, first_row, batch_blocks, 0)
        recv_nrm = lax.dynamic_slice_in_dim(recv_normals, first_row, batch_blocks, 0)
        transfer_factors = form_tiles(recv_pos, recv_nrm, jnp.take(src_positions, picked_rows, axis=0),
                             jnp.take(src_normals, picked_rows, axis=0), jnp.take(src_area, picked_rows, axis=0))
        collected_values = jnp.take(source_rows, picked_rows, axis=0)
        return jnp.einsum('wxmy,wxsy->wms', collected_values.astype(jnp.float32), transfer_factors.astype(jnp.float32))

    summed = lax.map(group_term, jnp.arange(turns, dtype=jnp.int32))
    return summed.reshape((pair_row_list.shape[0],) + source_rows.shape[1:])


def apply_albedo(summed, albedo):
    blocks_here, channels, verts = summed.shape
    shaped = summed.reshape(blocks_here, COLORS, channels // COLORS, verts) * albedo[:, :, None, :]
    return shaped.reshape(blocks_here, channels, verts)


def reference(transfer, positions, normals, area, albedo, pairs, home):
    slot_ids = jnp.take(home, pairs, axis=0)
    first_bounce = apply_albedo(reflect_all(transfer, positions, normals, area, slot_ids, positions, normals), albedo)
    bounce_one = first_bounce.astype(jnp.bfloat16)
    second_bounce = apply_albedo(reflect_all(bounce_one, positions, normals, area, slot_ids, positions, normals), albedo)
    bounce_two = second_bounce.astype(jnp.bfloat16)
    inv_count = 1.0 / (BLOCKS * VERT * CH)
    energy_one = jnp.sum(area[:, None, :] * first_bounce * first_bounce) * inv_count
    energy_two = jnp.sum(area[:, None, :] * second_bounce * second_bounce) * inv_count
    energies = jnp.stack([energy_one, energy_two]).astype(jnp.float32)
    return bounce_one, bounce_two, energies
```

```python
import functools
import itertools

import jax
import jax.numpy as jnp
import numpy as np
from jax import lax
from jax.experimental import pallas as pl
from jax.experimental.pallas import tpu as pltpu
from jax.sharding import Mesh
from jax.sharding import PartitionSpec as P

AX = ("y", "c", "z", "x")
SZ = (4, 2, 4, 4)
NDEV = 128
SLOTS, NEAR, FAR, CH, V = 16, 16, 24, 75, 128
ROWS = 80
F32, BF16, I32 = jnp.float32, jnp.bfloat16, jnp.int32
MESH = pl.DeviceIdType.MESH


def rounded(t):
    return t.astype(BF16).astype(F32)


def pieces3(t):
    a = rounded(t)
    b = rounded(t - a)
    return a, b, rounded(t - a - b)


def rows_of(shape):
    return lax.broadcasted_iota(I32, shape, 0)


def source_features(v):
    r = rows_of((8, V))
    vh = rounded(v)
    vl = rounded(v - vh)
    m = -(v * v[6:7])
    mh = rounded(m)
    ml = rounded(m - mh)
    x = jnp.where(r < 3, v, 0.0)
    c = pieces3(jnp.sum(pltpu.roll(m, 5, 0) * x, axis=0, keepdims=True))
    e = pieces3(jnp.sum(x * x, axis=0, keepdims=True) + 1.0)
    cv = jnp.ones((8, V), F32)
    for i, row in enumerate(c + e):
        cv = jnp.where(r == i, row, cv)
    return jnp.concatenate([vh, vh, vl, mh, mh, ml, cv, jnp.zeros((8, V), F32)], axis=0).astype(BF16)


def receiver_features(v):
    r = rows_of((8, V))
    z = jnp.zeros((8, V), F32)
    x = jnp.where(r < 3, v, 0.0)
    n = jnp.where(r < 3, pltpu.roll(v, 5, 0), 0.0) * (1.0 / np.pi)
    nh = rounded(n)
    nl = rounded(n - nh)
    xh = rounded(x)
    xl = rounded(x - xh)
    k = pieces3(-jnp.sum(n * x, axis=0, keepdims=True))
    q = pieces3(jnp.sum(x * x, axis=0, keepdims=True))
    xh3 = -pltpu.roll(xh, 3, 0)
    xl3 = -pltpu.roll(xl, 3, 0)
    last = r == 7
    ap = [jnp.where(last, k[0], nh), jnp.where(last, k[1], nl), nh, z, z, z, jnp.where(r == 6, k[2], z), z]
    aq = [z, z, z, xh3, xl3, xh3, jnp.where(r < 3, 1.0, z), z]
    d = [jnp.where(last, q[0], -2.0 * xh), jnp.where(last, q[1], -2.0 * xl), -2.0 * xh, z, z, z,
         jnp.where((r >= 3) & (r < 6), 1.0, jnp.where(r == 6, q[2], z)), z]
    ap, aq, d = (jnp.concatenate(t, axis=0).astype(BF16) for t in (ap, aq, d))
    o = jnp.zeros((64, V), BF16)
    top = jnp.concatenate([ap, aq, o, o, d, o], axis=1)
    bottom = jnp.concatenate([o, o, ap, aq, o, d], axis=1)
    return jnp.concatenate([top, bottom], axis=0)


def pair_factors(feats, recv):
    out = lax.dot_general(feats, recv, (((0,), (0,)), ((), ())), preferred_element_type=F32)
    parts = []
    for i in range(2):
        ap = out[:, 256 * i : 256 * i + 128]
        aq = out[:, 256 * i + 128 : 256 * i + 256]
        d = out[:, 512 + 128 * i : 640 + 128 * i]
        parts.append((jnp.maximum(ap, 0.0) * jnp.maximum(aq, 0.0) / (d * d)).astype(BF16))
    return jnp.concatenate(parts, axis=0)


def me4():
    return tuple(lax.axis_index(a) for a in AX)


def my_index():
    y, c, z, x = me4()
    return ((y * 2 + c) * 4 + z) * 4 + x


def shifted(off):
    return tuple(lax.rem(i + o, s) for i, o, s in zip(me4(), off, SZ))


def flat(t):
    return ((t[0] * 2 + t[1]) * 4 + t[2]) * 4 + t[3]


def index_kernel(pairs_ref, home_ref, idx_ref, req_ref):
    p = pairs_ref[...]
    home = home_ref[...]
    shape = (SLOTS, V)
    lane = lax.broadcasted_iota(I32, shape, 1)
    low, high = p & 127, p >> 7
    slot = jnp.zeros(shape, I32)
    for h in range(16):
        got = jnp.take_along_axis(jnp.broadcast_to(home[h : h + 1], shape), low, axis=1)
        slot = jnp.where(high == h, got, slot)
    owner, local = slot >> 4, slot & 15
    lo = jnp.full(shape, 99, I32)
    hi = jnp.full(shape, -1, I32)
    for j in range(NEAR, NEAR + FAR):
        same = owner[:, j : j + 1] == lane
        lo = jnp.where(same, jnp.minimum(lo, local[:, j : j + 1]), lo)
        hi = jnp.where(same, jnp.maximum(hi, local[:, j : j + 1]), hi)
    lo = jnp.min(lo, axis=0, keepdims=True)
    hi = jnp.max(hi, axis=0, keepdims=True)
    lo = jnp.where(lo > 15, 0, lo)
    hi = jnp.where(hi < 0, 0, hi)
    first = jnp.take_along_axis(jnp.broadcast_to(lo, shape), owner, axis=1)
    far = owner * 2 + jnp.where(local != first, 1, 0)
    idx_ref[...] = jnp.where(lane < NEAR, local, far)
    req_ref[...] = jnp.where(rows_of((2, V)) == 0, lo, hi)


OFFSETS = [o for o in itertools.product(range(4), range(2), range(4), range(4)) if any(o)]
ORDER = [OFFSETS[i] for i in np.random.RandomState(0).permutation(len(OFFSETS))]


def send_all(src_of, dst, send_sem, recv_sem):
    mine = my_index()
    for off in ORDER:
        to = shifted(off)
        pltpu.make_async_remote_copy(
            src_of(flat(to)), dst.at[mine], send_sem, recv_sem, device_id=to, device_id_type=MESH
        ).start()


def wait_all(buf, sem):
    part = buf.at[pl.ds(0, NDEV - 1)]
    pltpu.make_async_copy(part, part, sem).wait()


def main_kernel(
    idx, req_ref, tr_ref, geo_ref, alb_ref, b1_ref, b2_ref, en_ref,
    reqall, wanted, en_all, near_s, near_g, send_g, recv_g, send_s, recv_s, recv_s2,
    feats, factors, acc, send_sem, recv_sem, local_sem,
):
    send_all(lambda d: req_ref, reqall, send_sem.at[0], recv_sem.at[0])
    reqall[my_index()] = req_ref[...]
    en_all[my_index()] = jnp.zeros((8, V), F32)
    near_s[:, 64:, :] = jnp.zeros((SLOTS, ROWS - 64, V), BF16)
    near_s[:, :CH, :] = tr_ref[...]
    near_g[...] = geo_ref[...].astype(BF16)

    @pl.loop(0, SLOTS)
    def _(b):
        feats[2 * NDEV + b] = source_features(geo_ref[b])

    wait_all(reqall, recv_sem.at[0])
    mine = my_index()
    copy = pltpu.make_async_copy(reqall, wanted, local_sem)
    copy.start()
    copy.wait()

    @pl.loop(0, NDEV)
    def _(a):
        for h in range(2):
            send_g[a, h] = near_g[wanted[a, h, mine]]

    send_all(lambda d: send_g.at[d], recv_g, send_sem.at[1], recv_sem.at[1])

    def gather_s():
        @pl.loop(0, NDEV)
        def _(a):
            for h in range(2):
                send_s[a, h] = near_s[wanted[a, h, mine]]

    gather_s()
    send_all(lambda d: send_s.at[d], recv_s, send_sem.at[2], recv_sem.at[2])

    def build(first, count, base):
        @pl.loop(0, SLOTS)
        def _(s):
            recv = receiver_features(geo_ref[s])
            for jj in range(first // 2, (first + count) // 2):
                pair = [feats[base + idx[s, 2 * jj + i]] for i in range(2)]
                factors[s, jj] = pair_factors(jnp.concatenate(pair, axis=0), recv)

    def applied(load, s, first, count):
        total = None
        for jj in range(first // 2, (first + count) // 2):
            lhs = jnp.concatenate([load(idx[s, 2 * jj + i]) for i in range(2)], axis=1)
            term = jnp.dot(lhs, factors[s, jj], preferred_element_type=F32)
            total = term if total is None else total + term
        return total

    def near_apply():
        @pl.loop(0, SLOTS)
        def _(s):
            acc[s] = applied(lambda i: near_s[i], s, 0, NEAR)

    def far_apply(table, out_ref, row, keep):
        r = rows_of((ROWS, V))
        mark = rows_of((8, V)) == row

        @pl.loop(0, SLOTS)
        def _(s):
            total = acc[s] + applied(lambda i: table[i // 2, i % 2], s, NEAR, FAR)
            a = alb_ref[s]
            total = total * jnp.where(r < 25, a[0:1], jnp.where(r < 50, a[1:2], a[2:3]))
            value = total.astype(BF16)
            out_ref[s] = value[:CH]
            if keep:
                near_s[s] = value
            energy = jnp.sum(total * total * geo_ref[s][6:7], axis=0, keepdims=True)
            en_all[my_index()] += jnp.where(mark, energy, 0.0)

    build(0, NEAR, 2 * NDEV)
    near_apply()
    wait_all(recv_g, recv_sem.at[1])

    @pl.loop(0, NDEV)
    def _(a):
        for h in range(2):
            feats[2 * a + h] = source_features(recv_g[a, h].astype(F32))

    build(NEAR, FAR, 0)
    wait_all(recv_s, recv_sem.at[2])
    wait_all(send_s, send_sem.at[2])
    far_apply(recv_s, b1_ref, 0, True)
    gather_s()
    send_all(lambda d: send_s.at[d], recv_s2, send_sem.at[3], recv_sem.at[3])
    near_apply()
    wait_all(recv_s2, recv_sem.at[3])
    far_apply(recv_s2, b2_ref, 1, False)
    send_all(lambda d: en_all.at[mine], en_all, send_sem.at[4], recv_sem.at[4])
    wait_all(en_all, recv_sem.at[4])
    en_ref[...] = jnp.sum(en_all[...], axis=0)
    wait_all(en_all, send_sem.at[4])
    wait_all(send_s, send_sem.at[3])
    wait_all(send_g, send_sem.at[1])
    wait_all(reqall, send_sem.at[0])


def body(transfer, positions, normals, area, albedo, pairs, home):
    vm = pl.BlockSpec(memory_space=pltpu.VMEM)
    sm = pl.BlockSpec(memory_space=pltpu.SMEM)
    idx, req = pl.pallas_call(
        index_kernel,
        out_shape=(jax.ShapeDtypeStruct((SLOTS, V), I32), jax.ShapeDtypeStruct((2, V), I32)),
        in_specs=[vm, vm],
        out_specs=(vm, vm),
    )(jnp.pad(pairs, ((0, 0), (0, V - NEAR - FAR))), home.reshape(16, V))
    geo = jnp.concatenate([positions, normals, area[:, None], jnp.ones((SLOTS, 1, V), F32)], axis=1)
    dma = pltpu.SemaphoreType.DMA
    b1, b2, en = pl.pallas_call(
        main_kernel,
        out_shape=(
            jax.ShapeDtypeStruct((SLOTS, CH, V), BF16),
            jax.ShapeDtypeStruct((SLOTS, CH, V), BF16),
            jax.ShapeDtypeStruct((8, V), F32),
        ),
        in_specs=[sm, vm, vm, vm, vm],
        out_specs=(vm, vm, vm),
        scratch_shapes=[
            pltpu.VMEM((NDEV, 2, V), I32),
            pltpu.SMEM((NDEV, 2, V), I32),
            pltpu.VMEM((NDEV, 8, V), F32),
            pltpu.VMEM((SLOTS, ROWS, V), BF16),
            pltpu.VMEM((SLOTS, 8, V), BF16),
            pltpu.VMEM((NDEV, 2, 8, V), BF16),
            pltpu.VMEM((NDEV, 2, 8, V), BF16),
            pltpu.VMEM((NDEV, 2, ROWS, V), BF16),
            pltpu.VMEM((NDEV, 2, ROWS, V), BF16),
            pltpu.VMEM((NDEV, 2, ROWS, V), BF16),
            pltpu.VMEM((2 * NDEV + SLOTS, 64, V), BF16),
            pltpu.VMEM((SLOTS, (NEAR + FAR) // 2, 2 * V, V), BF16),
            pltpu.VMEM((SLOTS, ROWS, V), F32),
            dma((5,)), dma((5,)), dma,
        ],
        compiler_params=pltpu.CompilerParams(has_side_effects=True, vmem_limit_bytes=58 * 2**20),
    )(idx, req, transfer, geo, albedo)
    energies = jnp.sum(en[:2], axis=1) * (1.0 / (NDEV * SLOTS * CH * V))
    return b1, b2, energies


def solution(mesh):
    finer = Mesh(mesh.devices.reshape(SZ), AX)
    split = [P(AX, *([None] * n)) for n in (2, 2, 2, 1, 2, 1)]
    return jax.shard_map(
        body,
        mesh=finer,
        in_specs=(*split, P()),
        out_specs=(split[0], split[0], P()),
        check_vma=False,
    )
```

```python
import functools
import itertools

import jax
import jax.numpy as jnp
import numpy as np
from jax import lax
from jax.experimental import pallas as pl
from jax.experimental.pallas import tpu as pltpu
from jax.sharding import Mesh
from jax.sharding import PartitionSpec as P

AX = ("y", "c", "z", "x")
SZ = (4, 2, 4, 4)
NDEV = 128
SLOTS, NEAR, FAR, CH, V = 16, 16, 24, 75, 128
ROWS = 80
F32, BF16, I32 = jnp.float32, jnp.bfloat16, jnp.int32
MESH = pl.DeviceIdType.MESH


def rounded(t):
    return t.astype(BF16).astype(F32)


def pieces3(t):
    a = rounded(t)
    b = rounded(t - a)
    return a, b, rounded(t - a - b)


def rows_of(shape):
    return lax.broadcasted_iota(I32, shape, 0)


def source_features(v):
    r = rows_of((8, V))
    vh = rounded(v)
    vl = rounded(v - vh)
    m = -(v * v[6:7])
    mh = rounded(m)
    ml = rounded(m - mh)
    x = jnp.where(r < 3, v, 0.0)
    c = pieces3(jnp.sum(pltpu.roll(m, 5, 0) * x, axis=0, keepdims=True))
    e = pieces3(jnp.sum(x * x, axis=0, keepdims=True) + 1.0)
    cv = jnp.ones((8, V), F32)
    for i, row in enumerate(c + e):
        cv = jnp.where(r == i, row, cv)
    return jnp.concatenate([vh, vh, vl, mh, mh, ml, cv, jnp.zeros((8, V), F32)], axis=0).astype(BF16)


def receiver_features(v):
    r = rows_of((8, V))
    z = jnp.zeros((8, V), F32)
    x = jnp.where(r < 3, v, 0.0)
    n = jnp.where(r < 3, pltpu.roll(v, 5, 0), 0.0) * (1.0 / np.pi)
    nh = rounded(n)
    nl = rounded(n - nh)
    xh = rounded(x)
    xl = rounded(x - xh)
    k = pieces3(-jnp.sum(n * x, axis=0, keepdims=True))
    q = pieces3(jnp.sum(x * x, axis=0, keepdims=True))
    xh3 = -pltpu.roll(xh, 3, 0)
    xl3 = -pltpu.roll(xl, 3, 0)
    last = r == 7
    ap = [jnp.where(last, k[0], nh), jnp.where(last, k[1], nl), nh, z, z, z, jnp.where(r == 6, k[2], z), z]
    aq = [z, z, z, xh3, xl3, xh3, jnp.where(r < 3, 1.0, z), z]
    d = [jnp.where(last, q[0], -2.0 * xh), jnp.where(last, q[1], -2.0 * xl), -2.0 * xh, z, z, z,
         jnp.where((r >= 3) & (r < 6), 1.0, jnp.where(r == 6, q[2], z)), z]
    ap, aq, d = (jnp.concatenate(t, axis=0).astype(BF16) for t in (ap, aq, d))
    o = jnp.zeros((64, V), BF16)
    top = jnp.concatenate([ap, aq, o, o, d, o], axis=1)
    bottom = jnp.concatenate([o, o, ap, aq, o, d], axis=1)
    return jnp.concatenate([top, bottom], axis=0)


def pair_factors(feats, recv):
    out = lax.dot_general(feats, recv, (((0,), (0,)), ((), ())), preferred_element_type=F32)
    parts = []
    for i in range(2):
        ap = out[:, 256 * i : 256 * i + 128]
        aq = out[:, 256 * i + 128 : 256 * i + 256]
        d = out[:, 512 + 128 * i : 640 + 128 * i]
        parts.append((jnp.maximum(ap, 0.0) * jnp.maximum(aq, 0.0) / (d * d)).astype(BF16))
    return jnp.concatenate(parts, axis=0)


def me4():
    return tuple(lax.axis_index(a) for a in AX)


def my_index():
    y, c, z, x = me4()
    return ((y * 2 + c) * 4 + z) * 4 + x


def shifted(off):
    return tuple(lax.rem(i + o, s) for i, o, s in zip(me4(), off, SZ))


def flat(t):
    return ((t[0] * 2 + t[1]) * 4 + t[2]) * 4 + t[3]


def index_kernel(pairs_ref, home_ref, idx_ref, req_ref):
    p = pairs_ref[...]
    home = home_ref[...]
    shape = (SLOTS, V)
    lane = lax.broadcasted_iota(I32, shape, 1)
    low, high = p & 127, p >> 7
    slot = jnp.zeros(shape, I32)
    for h in range(16):
        got = jnp.take_along_axis(jnp.broadcast_to(home[h : h + 1], shape), low, axis=1)
        slot = jnp.where(high == h, got, slot)
    owner, local = slot >> 4, slot & 15
    lo = jnp.full(shape, 99, I32)
    hi = jnp.full(shape, -1, I32)
    for j in range(NEAR, NEAR + FAR):
        same = owner[:, j : j + 1] == lane
        lo = jnp.where(same, jnp.minimum(lo, local[:, j : j + 1]), lo)
        hi = jnp.where(same, jnp.maximum(hi, local[:, j : j + 1]), hi)
    lo = jnp.min(lo, axis=0, keepdims=True)
    hi = jnp.max(hi, axis=0, keepdims=True)
    lo = jnp.where(lo > 15, 0, lo)
    hi = jnp.where(hi < 0, 0, hi)
    first = jnp.take_along_axis(jnp.broadcast_to(lo, shape), owner, axis=1)
    far = owner * 2 + jnp.where(local != first, 1, 0)
    idx_ref[...] = jnp.where(lane < NEAR, local, far)
    req_ref[...] = jnp.where(rows_of((2, V)) == 0, lo, hi)


OFFSETS = [o for o in itertools.product(range(4), range(2), range(4), range(4)) if any(o)]
ORDER = [OFFSETS[i] for i in np.random.RandomState(0).permutation(len(OFFSETS))]

DIMS = (0, 2, 3)
PLANES = ((2, 3), (0, 3), (0, 2))
SEG = 24
GEO = ((0, 1, 2), (3, 4), (5, 6))


def hops(off):
    return sum(min(off[d], 4 - off[d]) for d in DIMS)


def moved(dim, by):
    off = [0, 0, 0, 0]
    off[dim] = by
    return tuple(off)


def plane_offsets(k):
    a, b = PLANES[k]
    out = []
    for i, j, c in itertools.product(range(4), range(4), range(2)):
        off = [0, c, 0, 0]
        off[a], off[b] = i, j
        if any(off):
            out.append(tuple(off))
    order = np.random.RandomState(k).permutation(len(out))
    return sorted((out[i] for i in order), key=lambda o: -hops(o))


def plane_index(k, t):
    a, b = PLANES[k]
    return (t[b] * 4 + t[a]) * 2 + t[1]


def send(src, dst, send_sem, recv_sem, to):
    pltpu.make_async_remote_copy(
        src, dst, send_sem, recv_sem, device_id=to, device_id_type=MESH
    ).start()


def wait_for(part, sem):
    pltpu.make_async_copy(part, part, sem).wait()


def row_column(shape):
    return rows_of(shape), lax.broadcasted_iota(I32, shape, 1)


def selection(k, table):
    r, m = row_column((256, 64))
    expand = jnp.where(m == ((r >> 3) << 1) + (r & 1), 1.0, 0.0).astype(BF16)
    wide = jnp.dot(expand, table.astype(F32).astype(BF16), preferred_element_type=F32)
    r, lane = row_column((256, V))
    coords = list(me4())
    coords[DIMS[k]] = (r >> 1) & 3
    value = jnp.sum(jnp.where(lane == flat(coords), wide, 0.0), axis=1, keepdims=True)
    place = (lane - (((r >> 1) & 3) << 4)).astype(F32)
    return jnp.where(value == place, 1.0, 0.0)[:, :64].astype(BF16)


def canonical(k):
    r, col = row_column((256, 256))
    t = (r >> 6, (r >> 5) & 1, (r >> 3) & 3, (r >> 1) & 3)
    place = (plane_index(k, t) << 3) + (t[DIMS[k]] << 1) + (r & 1)
    return jnp.where(place == col, 1.0, 0.0).astype(BF16)


def main_kernel(
    idx, req_ref, tr_ref, geo_ref, alb_ref, b1_ref, b2_ref, en_ref,
    r0, r1, r2, wanted, near_s, la0, la1, la2, lb0, lb1, lb2, lc0, lc1, lc2, lr, sel,
    sg0, sg1, sg2, rg0, rg1, rg2, sr, rr, ss, tab_a, tab_b, geo_t, rem_t, tail,
    feats, factors, acc, en_all, sem_r, sem_rs, sem_b, sem_bs, sem_c, sem_cs, sem_u, sem_us,
    sem_g, sem_gs, sem_e, local_sem,
):
    lc, sg, rg = (lc0, lc1, lc2), (sg0, sg1, sg2), (rg0, rg1, rg2)
    line_a, line_b = (la0, la1, la2), (lb0, lb1, lb2)
    here = me4()
    core = here[1]
    pos = [here[d] for d in DIMS]
    partner = shifted((0, 1, 0, 0))
    lines = [[shifted(moved(d, by)) for by in (2, 1, 3)] for d in DIMS]

    barrier = pltpu.get_barrier_semaphore()
    for to in [partner] + sum(lines, []):
        pl.semaphore_signal(barrier, inc=1, device_id=to, device_id_type=MESH)
    near_s[:, 64:, :] = jnp.zeros((SLOTS, ROWS - 64, V), BF16)
    near_s[:, :CH, :] = tr_ref[...]
    r0[core] = req_ref[...]

    def fill_lines(line):
        for k in range(3):
            line[k][pos[k]] = near_s[:, SEG * k : SEG * (k + 1), :]

    def rem_rows(k):
        rows = near_s[:, 72:80, :].astype(F32)
        return rows[:, k, :].astype(BF16)

    fill_lines(line_a)
    for k in range(3):
        lc[k][pos[k], 0] = rem_rows(k)
        for g, comp in enumerate(GEO[k]):
            lc[k][pos[k], 1 + g] = geo_ref[:, comp, :].astype(BF16)
    pl.semaphore_wait(barrier, 10)

    send(req_ref, r0.at[core], sem_rs.at[0], sem_r.at[0], partner)

    def send_lines(line, n):
        for by in range(3):
            for k in range(3):
                part = line[k].at[pos[k]]
                send(part, part, sem_bs.at[n, k], sem_b.at[n, k], lines[k][by])

    for by in range(3):
        for k in range(3):
            part = lc[k].at[pos[k]]
            send(part, part, sem_cs.at[0, k], sem_c.at[0, k], lines[k][by])
    wait_for(r0.at[0], sem_r.at[0])
    for i in range(3):
        r1[i, pl.ds(pos[i] * 2, 2)] = r0[...]
        for to in lines[i]:
            send(r0, r1.at[i, pl.ds(pos[i] * 2, 2)], sem_rs.at[1 + i], sem_r.at[1 + i], to)
    send_lines(line_a, 0)
    for i in range(3):
        wait_for(r1.at[i, pl.ds(0, 6)], sem_r.at[1 + i])
    for k in range(3):
        ia, ib = (DIMS.index(d) for d in PLANES[k])
        part = r2.at[k, pl.ds(pos[ib] * 8, 8)]
        r2[k, pl.ds(pos[ib] * 8, 8)] = r1[ia]
        for to in lines[ib]:
            send(r1.at[ia], part, sem_rs.at[4 + k], sem_r.at[4 + k], to)

    rem_t[...] = jnp.zeros((2 * NDEV, 8, V), F32)
    geo_t[:, 7, :] = jnp.ones((2 * NDEV, V), F32)
    en_all[my_index()] = jnp.zeros((2, V), F32)

    @pl.loop(0, SLOTS)
    def _(b):
        feats[2 * NDEV + b] = source_features(geo_ref[b])

    for k in range(3):
        wait_for(r2.at[k, pl.ds(0, 24)], sem_r.at[4 + k])
    copy = pltpu.make_async_copy(r2, wanted, local_sem)
    copy.start()
    for k in range(3):
        table = jnp.concatenate([r2[k, i] for i in range(32)], axis=0)
        sel[k] = selection(k, table)
    copy.wait()

    for k in range(3):
        wait_for(lc[k].at[pl.ds(0, 3)], sem_c.at[0, k])
        for g in range(1 + len(GEO[k])):
            source = lc[k][:, g].reshape(64, V)
            got = jnp.dot(sel[k], source, preferred_element_type=F32).astype(BF16)
            sg[k][:, g] = got.reshape(32, 8, V)
        mine = plane_index(k, here)
        rg[k][mine] = sg[k][mine]
        for off in plane_offsets(k):
            to = shifted(off)
            send(sg[k].at[plane_index(k, to)], rg[k].at[mine], sem_gs.at[0, k], sem_g.at[0, k], to)

    def owner_slice(ref, k, t):
        at = [t[0], t[1], t[2], t[3]]
        at[DIMS[k]] = slice(None)
        return ref.at[at[0], at[1], at[2], at[3], :, pl.ds(SEG * k, SEG), :]

    def spread(line, tab, n):
        for k in range(3):
            wait_for(line[k].at[pl.ds(0, 3)], sem_b.at[n, k])
            owners = []
            for o in range(4):
                t = list(here)
                t[DIMS[k]] = o
                owners.append(t)
            flat_owner = [flat(t) for t in owners]

            @pl.loop(0, 32)
            def _(d):
                for o in range(4):
                    for h in range(2):
                        ss[k, d, o, h] = line[k][o, wanted[k, d, h, flat_owner[o]]]

            mine = plane_index(k, here)
            for o in range(4):
                t = owners[o]
                for h in range(2):
                    block = line[k][o, wanted[k, mine, h, flat_owner[o]]]
                    tab[t[0], t[1], t[2], t[3], h, SEG * k : SEG * (k + 1), :] = block
            for off in plane_offsets(k):
                to = shifted(off)
                send(ss.at[k, plane_index(k, to)], owner_slice(tab, k, here),
                     sem_us.at[n, k], sem_u.at[n, k], to)

    spread(line_a, tab_a, 0)

    def build(first, count, base):
        @pl.loop(0, SLOTS)
        def _(s):
            recv = receiver_features(geo_ref[s])
            for jj in range(first // 2, (first + count) // 2):
                pair = [feats[base + idx[s, 2 * jj + i]] for i in range(2)]
                factors[s, jj] = pair_factors(jnp.concatenate(pair, axis=0), recv)

    def applied(load, s, first, count):
        total = None
        for jj in range(first // 2, (first + count) // 2):
            lhs = jnp.concatenate([load(idx[s, 2 * jj + i]) for i in range(2)], axis=1)
            term = jnp.dot(lhs, factors[s, jj], preferred_element_type=F32)
            total = term if total is None else total + term
        return total

    def near_apply():
        @pl.loop(0, SLOTS)
        def _(s):
            acc[s] = applied(lambda i: near_s[i], s, 0, NEAR)

    def far_apply(tab, out_ref, row):
        r = rows_of((ROWS, V))
        mark = rows_of((2, V)) == row

        def load(i):
            head = tab[i >> 6, (i >> 5) & 1, (i >> 3) & 3, (i >> 1) & 3, i & 1]
            return jnp.concatenate([head, tail[i]], axis=0)

        @pl.loop(0, SLOTS)
        def _(s):
            total = acc[s] + applied(load, s, NEAR, FAR)
            a = alb_ref[s]
            total = total * jnp.where(r < 25, a[0:1], jnp.where(r < 50, a[1:2], a[2:3]))
            value = total.astype(BF16)
            out_ref[s] = value[:CH]
            if row == 0:
                near_s[s] = value
            energy = jnp.sum(total * total * geo_ref[s][6:7], axis=0, keepdims=True)
            en_all[my_index()] += jnp.where(mark, energy, 0.0)

    def tails(rows_of_part):
        for k in range(3):
            rem_t[:, k, :] = jnp.dot(canonical(k), rows_of_part(k), preferred_element_type=F32)
        tail[...] = rem_t[...].astype(BF16)

    build(0, NEAR, 2 * NDEV)
    near_apply()
    for k in range(3):
        wait_for(rg[k].at[pl.ds(0, 31)], sem_g.at[0, k])
        order = canonical(k)
        for g, comp in enumerate(GEO[k]):
            rows = rg[k][:, 1 + g].reshape(256, V)
            geo_t[:, comp, :] = jnp.dot(order, rows, preferred_element_type=F32)
    tails(lambda k: rg[k][:, 0].reshape(256, V))

    @pl.loop(0, 2 * NDEV)
    def _(b):
        feats[b] = source_features(geo_t[b])

    build(NEAR, FAR, 0)
    for k in range(3):
        wait_for(ss.at[k, pl.ds(0, 31)], sem_u.at[0, k])
    far_apply(tab_a, b1_ref, 0)

    fill_lines(line_b)
    for k in range(3):
        lr[k, pos[k]] = rem_rows(k)
    for by in range(3):
        for k in range(3):
            part = lr.at[k, pos[k]]
            send(part, part, sem_cs.at[1, k], sem_c.at[1, k], lines[k][by])
    send_lines(line_b, 1)
    near_apply()
    for k in range(3):
        wait_for(ss.at[k, pl.ds(0, 31)], sem_us.at[0, k])
        wait_for(lr.at[k, pl.ds(0, 3)], sem_c.at[1, k])
        got = jnp.dot(sel[k], lr[k].reshape(64, V), preferred_element_type=F32).astype(BF16)
        sr[k] = got.reshape(32, 8, V)
        mine = plane_index(k, here)
        rr[k, mine] = sr[k, mine]
        for off in plane_offsets(k):
            to = shifted(off)
            send(sr.at[k, plane_index(k, to)], rr.at[k, mine], sem_gs.at[1, k], sem_g.at[1, k], to)
    spread(line_b, tab_b, 1)
    for k in range(3):
        wait_for(rr.at[k, pl.ds(0, 31)], sem_g.at[1, k])
    tails(lambda k: rr[k].reshape(256, V))
    for k in range(3):
        wait_for(ss.at[k, pl.ds(0, 31)], sem_u.at[1, k])
    far_apply(tab_b, b2_ref, 1)

    mine = my_index()
    for off in ORDER:
        send(en_all.at[mine], en_all.at[mine], sem_e.at[0], sem_e.at[1], shifted(off))
    wait_for(en_all.at[pl.ds(0, NDEV - 1)], sem_e.at[1])
    en_ref[...] = jnp.sum(en_all[...], axis=0)
    wait_for(en_all.at[pl.ds(0, NDEV - 1)], sem_e.at[0])
    wait_for(r0.at[0], sem_rs.at[0])
    for i in range(3):
        wait_for(r1.at[i, pl.ds(0, 6)], sem_rs.at[1 + i])
        wait_for(r2.at[i, pl.ds(0, 24)], sem_rs.at[4 + i])
        wait_for(lc[i].at[pl.ds(0, 3)], sem_cs.at[0, i])
        wait_for(lr.at[i, pl.ds(0, 3)], sem_cs.at[1, i])
        wait_for(rg[i].at[pl.ds(0, 31)], sem_gs.at[0, i])
        wait_for(rr.at[i, pl.ds(0, 31)], sem_gs.at[1, i])
        wait_for(ss.at[i, pl.ds(0, 31)], sem_us.at[1, i])
        for n, line in enumerate((line_a, line_b)):
            wait_for(line[i].at[pl.ds(0, 3)], sem_bs.at[n, i])


def body(transfer, positions, normals, area, albedo, pairs, home):
    vm = pl.BlockSpec(memory_space=pltpu.VMEM)
    sm = pl.BlockSpec(memory_space=pltpu.SMEM)
    idx, req = pl.pallas_call(
        index_kernel,
        out_shape=(jax.ShapeDtypeStruct((SLOTS, V), I32), jax.ShapeDtypeStruct((2, V), I32)),
        in_specs=[vm, vm],
        out_specs=(vm, vm),
    )(jnp.pad(pairs, ((0, 0), (0, V - NEAR - FAR))), home.reshape(16, V))
    geo = jnp.concatenate([positions, normals, area[:, None], jnp.ones((SLOTS, 1, V), F32)], axis=1)
    dma = pltpu.SemaphoreType.DMA
    b1, b2, en = pl.pallas_call(
        main_kernel,
        out_shape=(
            jax.ShapeDtypeStruct((SLOTS, CH, V), BF16),
            jax.ShapeDtypeStruct((SLOTS, CH, V), BF16),
            jax.ShapeDtypeStruct((2, V), F32),
        ),
        in_specs=[sm, vm, vm, vm, vm],
        out_specs=(vm, vm, vm),
        scratch_shapes=[
            pltpu.VMEM((2, 2, V), I32),
            pltpu.VMEM((3, 8, 2, V), I32),
            pltpu.VMEM((3, 32, 2, V), I32),
            pltpu.SMEM((3, 32, 2, V), I32),
            pltpu.VMEM((SLOTS, ROWS, V), BF16),
            *[pltpu.VMEM((4, SLOTS, SEG, V), BF16) for _ in range(6)],
            *[pltpu.VMEM((4, 1 + len(g), SLOTS, V), BF16) for g in GEO],
            pltpu.VMEM((3, 4, SLOTS, V), BF16),
            pltpu.VMEM((3, 256, 64), BF16),
            *[pltpu.VMEM((32, 1 + len(g), 8, V), BF16) for g in GEO],
            *[pltpu.VMEM((32, 1 + len(g), 8, V), BF16) for g in GEO],
            pltpu.VMEM((3, 32, 8, V), BF16),
            pltpu.VMEM((3, 32, 8, V), BF16),
            pltpu.VMEM((3, 32, 4, 2, SEG, V), BF16),
            pltpu.VMEM((4, 2, 4, 4, 2, 3 * SEG, V), BF16),
            pltpu.VMEM((4, 2, 4, 4, 2, 3 * SEG, V), BF16),
            pltpu.VMEM((2 * NDEV, 8, V), F32),
            pltpu.VMEM((2 * NDEV, 8, V), F32),
            pltpu.VMEM((2 * NDEV, 8, V), BF16),
            pltpu.VMEM((2 * NDEV + SLOTS, 64, V), BF16),
            pltpu.VMEM((SLOTS, (NEAR + FAR) // 2, 2 * V, V), BF16),
            pltpu.VMEM((SLOTS, ROWS, V), F32),
            pltpu.VMEM((NDEV, 2, V), F32),
            dma((7,)), dma((7,)), dma((2, 3)), dma((2, 3)), dma((2, 3)), dma((2, 3)),
            dma((2, 3)), dma((2, 3)), dma((2, 3)), dma((2, 3)), dma((2,)), dma,
        ],
        compiler_params=pltpu.CompilerParams(collective_id=0, has_side_effects=True, vmem_limit_bytes=58 * 2**20),
    )(idx, req, transfer, geo, albedo)
    energies = jnp.sum(en, axis=1) * (1.0 / (NDEV * SLOTS * CH * V))
    return b1, b2, energies


def solution(mesh):
    finer = Mesh(mesh.devices.reshape(SZ), AX)
    split = [P(AX, *([None] * n)) for n in (2, 2, 2, 1, 2, 1)]
    return jax.shard_map(
        body,
        mesh=finer,
        in_specs=(*split, P()),
        out_specs=(split[0], split[0], P()),
        check_vma=False,
    )
```

```python
import itertools
import types

import jax
import jax.numpy as jnp
import numpy as np
from jax import lax
from jax.experimental import pallas as pl
from jax.experimental.pallas import tpu as pltpu
from jax.sharding import Mesh
from jax.sharding import PartitionSpec as P

AX = ("y", "c", "z", "x")
SZ = (4, 2, 4, 4)
NDEV = 128
SLOTS, NEAR, FAR, CH, V = 16, 16, 24, 75, 128
ROWS = 80
F32, BF16, I32 = jnp.float32, jnp.bfloat16, jnp.int32
MESH = pl.DeviceIdType.MESH


def rounded(t):
    return t.astype(BF16).astype(F32)


def pieces3(t):
    a = rounded(t)
    b = rounded(t - a)
    return a, b, rounded(t - a - b)


def rows_of(shape):
    return lax.broadcasted_iota(I32, shape, 0)


def source_features(v):
    r = rows_of((8, V))
    vh = rounded(v)
    vl = rounded(v - vh)
    m = -(v * v[6:7])
    mh = rounded(m)
    ml = rounded(m - mh)
    x = jnp.where(r < 3, v, 0.0)
    c = pieces3(jnp.sum(pltpu.roll(m, 5, 0) * x, axis=0, keepdims=True))
    e = pieces3(jnp.sum(x * x, axis=0, keepdims=True) + 1.0)
    cv = jnp.ones((8, V), F32)
    for i, row in enumerate(c + e):
        cv = jnp.where(r == i, row, cv)
    return jnp.concatenate([vh, vh, vl, mh, mh, ml, cv, jnp.zeros((8, V), F32)], axis=0).astype(BF16)


def receiver_features(v):
    r = rows_of((8, V))
    z = jnp.zeros((8, V), F32)
    x = jnp.where(r < 3, v, 0.0)
    n = jnp.where(r < 3, pltpu.roll(v, 5, 0), 0.0) * (1.0 / np.pi)
    nh = rounded(n)
    nl = rounded(n - nh)
    xh = rounded(x)
    xl = rounded(x - xh)
    k = pieces3(-jnp.sum(n * x, axis=0, keepdims=True))
    q = pieces3(jnp.sum(x * x, axis=0, keepdims=True))
    xh3 = -pltpu.roll(xh, 3, 0)
    xl3 = -pltpu.roll(xl, 3, 0)
    last = r == 7
    ap = [jnp.where(last, k[0], nh), jnp.where(last, k[1], nl), nh, z, z, z, jnp.where(r == 6, k[2], z), z]
    aq = [z, z, z, xh3, xl3, xh3, jnp.where(r < 3, 1.0, z), z]
    d = [jnp.where(last, q[0], -2.0 * xh), jnp.where(last, q[1], -2.0 * xl), -2.0 * xh, z, z, z,
         jnp.where((r >= 3) & (r < 6), 1.0, jnp.where(r == 6, q[2], z)), z]
    ap, aq, d = (jnp.concatenate(t, axis=0).astype(BF16) for t in (ap, aq, d))
    o = jnp.zeros((64, V), BF16)
    top = jnp.concatenate([ap, aq, o, o, d, o], axis=1)
    bottom = jnp.concatenate([o, o, ap, aq, o, d], axis=1)
    return jnp.concatenate([top, bottom], axis=0)


def pair_factors(feats, recv):
    out = lax.dot_general(feats, recv, (((0,), (0,)), ((), ())), preferred_element_type=F32)
    parts = []
    for i in range(2):
        ap = out[:, 256 * i : 256 * i + 128]
        aq = out[:, 256 * i + 128 : 256 * i + 256]
        d = out[:, 512 + 128 * i : 640 + 128 * i]
        parts.append((jnp.maximum(ap, 0.0) * jnp.maximum(aq, 0.0) / (d * d)).astype(BF16))
    return jnp.concatenate(parts, axis=0)


def me4():
    return tuple(lax.axis_index(a) for a in AX)


def my_index():
    y, c, z, x = me4()
    return ((y * 2 + c) * 4 + z) * 4 + x


def shifted(off):
    return tuple(lax.rem(i + o, s) for i, o, s in zip(me4(), off, SZ))


def flat(t):
    return ((t[0] * 2 + t[1]) * 4 + t[2]) * 4 + t[3]


def index_kernel(pairs_ref, home_ref, idx_ref, req_ref, wide_ref):
    wide_ref[...] = jnp.zeros((SLOTS, V), I32)
    wide_ref[:, : NEAR + FAR] = pairs_ref[...]
    p = wide_ref[...]
    home = home_ref[...]
    shape = (SLOTS, V)
    lane = lax.broadcasted_iota(I32, shape, 1)
    low, high = p & 127, p >> 7
    slot = jnp.zeros(shape, I32)
    for h in range(16):
        got = jnp.take_along_axis(jnp.broadcast_to(home[h : h + 1], shape), low, axis=1)
        slot = jnp.where(high == h, got, slot)
    owner, local = slot >> 4, slot & 15
    lo = jnp.full(shape, 99, I32)
    hi = jnp.full(shape, -1, I32)
    for j in range(NEAR, NEAR + FAR):
        same = owner[:, j : j + 1] == lane
        lo = jnp.where(same, jnp.minimum(lo, local[:, j : j + 1]), lo)
        hi = jnp.where(same, jnp.maximum(hi, local[:, j : j + 1]), hi)
    lo = jnp.min(lo, axis=0, keepdims=True)
    hi = jnp.max(hi, axis=0, keepdims=True)
    lo = jnp.where(lo > 15, 0, lo)
    hi = jnp.where(hi < 0, 0, hi)
    first = jnp.take_along_axis(jnp.broadcast_to(lo, shape), owner, axis=1)
    far = owner * 2 + jnp.where(local != first, 1, 0)
    idx_ref[...] = jnp.where(lane < NEAR, local, far)
    req_ref[...] = jnp.where(rows_of((2, V)) == 0, lo, hi)


OFFSETS = [o for o in itertools.product(range(4), range(2), range(4), range(4)) if any(o)]
ORDER = [OFFSETS[i] for i in np.random.RandomState(0).permutation(len(OFFSETS))]

DIMS = (0, 2, 3)
AXES = ((0, 2, 3), (2, 3, 0), (3, 0, 2))
STEPS = (2, 1, 3)
SEG = 24
GEO = ((0, 1, 2), (3, 4), (5, 6))
FROM = (0, 3, 2, 1)


def moved(dim, by, core=0):
    off = [0, core, 0, 0]
    off[dim] = by
    return tuple(off)


def send(src, dst, send_sem, recv_sem, to):
    pltpu.make_async_remote_copy(
        src, dst, send_sem, recv_sem, device_id=to, device_id_type=MESH
    ).start()


def wait_for(part, sem):
    pltpu.make_async_copy(part, part, sem).wait()


def row_column(shape):
    return rows_of(shape), lax.broadcasted_iota(I32, shape, 1)


def selection(k, table):
    here = me4()
    a, b, _ = AXES[k]
    r, m = row_column((256, 16))
    expand = jnp.where(m == ((r >> 5) << 1) + (r & 1), 1.0, 0.0).astype(BF16)
    wide = jnp.dot(expand, table.astype(F32).astype(BF16), preferred_element_type=F32)
    r, lane = row_column((256, V))
    coords = list(here)
    coords[a] = (here[a] + ((r >> 1) & 3)) & 3
    coords[b] = (here[b] + ((r >> 3) & 3)) & 3
    value = jnp.sum(jnp.where(lane == flat(coords), wide, 0.0), axis=1, keepdims=True)
    r, lane = row_column((256, 256))
    place = (lane - (((r >> 1) & 15) << 4)).astype(F32)
    return jnp.where(value == place, 1.0, 0.0).astype(BF16)


def canonical(k):
    here = me4()
    a, b, c = AXES[k]
    r, col = row_column((256, 256))
    t = (r >> 6, (r >> 5) & 1, (r >> 3) & 3, (r >> 1) & 3)
    i = (t[a] - here[a]) & 3
    j = (t[b] - here[b]) & 3
    place = (((t[c] << 1) + t[1]) << 5) + (j << 3) + (i << 1) + (r & 1)
    return jnp.where(place == col, 1.0, 0.0).astype(BF16)


def main_kernel(idx, req_ref, tr_ref, pos_ref, nrm_ref, area_ref, alb_ref, b1_ref, b2_ref, en_ref, *scratch):
    w = types.SimpleNamespace(**dict(zip([n for n, _ in scratch_list()], scratch)))
    factors, feats, acc, near_s = w.factors, w.feats, w.acc, w.near_s
    cp, sg, rg = (w.cp0, w.cp1, w.cp2), (w.sg0, w.sg1, w.sg2), (w.rg0, w.rg1, w.rg2)
    planes = [[[getattr(w, f"p{n}{k}{j}") for j in range(4)] for k in range(3)] for n in range(2)]
    tabs = (w.tab_a, w.tab_b)
    here = me4()
    core = here[1]
    mine = my_index()
    partner = shifted((0, 1, 0, 0))
    line = {d: {by: shifted(moved(d, by)) for by in STEPS} for d in DIMS}
    other = {d: {by: shifted(moved(d, by, 1)) for by in STEPS} for d in DIMS}

    barrier = pltpu.get_barrier_semaphore()
    greeted = [partner] + [t[d][by] for t in (line, other) for d in DIMS for by in STEPS]
    for to in greeted:
        pl.semaphore_signal(barrier, inc=1, device_id=to, device_id_type=MESH)

    for i in range(3):
        w.r1[i, here[DIMS[i]] * 2 + core] = req_ref[...]
    w.wide[:CH] = tr_ref[...].astype(F32)
    w.wide[CH:] = jnp.zeros((ROWS - CH, SLOTS, V), F32)
    comps = [pos_ref.at[0], pos_ref.at[1], pos_ref.at[2], nrm_ref.at[0], nrm_ref.at[1], nrm_ref.at[2], area_ref]
    for i, comp in enumerate(comps):
        w.geo[:, i, :] = comp[...]
    w.geo[:, 7, :] = jnp.ones((SLOTS, V), F32)
    for s in range(SLOTS):
        value = w.wide[:, s, :].astype(BF16)
        near_s[s] = value
        for k in range(3):
            planes[0][k][0][0, s] = value[SEG * k : SEG * (k + 1)]
    for k in range(3):
        cp[k][0, 0, 0] = tr_ref[72 + k]
        for g, comp in enumerate(GEO[k]):
            cp[k][0, 0, 1 + g] = comps[comp][...].astype(BF16)
    pl.semaphore_wait(barrier, len(greeted))

    for i in range(3):
        slot = w.r1.at[i, here[DIMS[i]] * 2 + core]
        for to in [line[DIMS[i]][by] for by in STEPS] + [other[DIMS[i]][by] for by in STEPS] + [partner]:
            send(req_ref, slot, w.sem_rs.at[i], w.sem_r.at[i], to)

    def first_leg(refs, send_sem, recv_sem):
        for by in STEPS:
            for k in range(3):
                send(refs[k].at[0], refs[k].at[FROM[by]], send_sem.at[k], recv_sem.at[k], line[AXES[k][0]][by])

    first_leg([c.at[0] for c in cp], w.sem_c1s, w.sem_c1)
    first_leg([p[0] for p in planes[0]], w.sem_b1s.at[0], w.sem_b1.at[0])

    def second_leg(n, part, size):
        for by in STEPS:
            for k in range(3):
                send(planes[n][k][0].at[pl.ds(part, size)], planes[n][k][FROM[by]].at[pl.ds(part, size)],
                     w.sem_b2s.at[n, k], w.sem_b2.at[n, k, FROM[by]], line[AXES[k][1]][by])

    def lines_second_leg(refs, send_sem, recv_sem):
        for by in STEPS:
            for k in range(3):
                send(refs[k].at[0], refs[k].at[FROM[by]], send_sem.at[k], recv_sem.at[k], line[AXES[k][1]][by])

    for k in range(3):
        wait_for(cp[k].at[0, pl.ds(0, 3)], w.sem_c1.at[k])
    lines_second_leg(cp, w.sem_c2s, w.sem_c2)
    second_leg(0, 0, 1)

    w.rem_t[...] = jnp.zeros((2 * NDEV, 8, V), F32)
    w.geo_t[:, 7, :] = jnp.ones((2 * NDEV, V), F32)
    w.en_all[mine] = jnp.zeros((2, V), F32)
    for i in range(3):
        wait_for(w.r1.at[i, pl.ds(0, 7)], w.sem_r.at[i])
    copy = pltpu.make_async_copy(w.r1, w.wanted, w.local_sem)
    copy.start()
    for k in range(3):
        i = DIMS.index(AXES[k][2])
        w.sel[k] = selection(k, jnp.concatenate([w.r1[i, d] for d in range(8)], axis=0))

    def ends(k):
        c = AXES[k][2]
        return [shifted(moved(c, by, o)) for by, o in ((2, 0), (2, 1), (1, 0), (1, 1), (3, 0), (3, 1), (0, 1))]

    def end_index(k, t):
        return t[AXES[k][2]] * 2 + t[1]

    for k in range(3):
        wait_for(cp[k].at[pl.ds(0, 3)], w.sem_c2.at[k])
        for g in range(1 + len(GEO[k])):
            source = cp[k][:, :, g].reshape(256, V)
            got = jnp.dot(w.sel[k], source, preferred_element_type=F32).astype(BF16)
            sg[k][:, g] = got.reshape(8, 32, V)
        me = end_index(k, here)
        rg[k][me] = sg[k][me]
        for to in ends(k):
            send(sg[k].at[end_index(k, to)], rg[k].at[me], w.sem_gs.at[0, k], w.sem_g.at[0, k], to)
    copy.wait()

    def first_leg_done(n):
        for k in range(3):
            wait_for(planes[n][k][0].at[pl.ds(0, 3)], w.sem_b1.at[n, k])
        second_leg(n, 1, 3)

    def spread(n, j):
        for k in range(3):
            a, b, c = AXES[k]
            wi = DIMS.index(c)
            plane = planes[n][k][j]
            if j:
                wait_for(plane, w.sem_b2.at[n, k, j])
            owners = []
            for i in range(4):
                t = list(here)
                t[a] = (here[a] + i) & 3
                t[b] = (here[b] + j) & 3
                owners.append((t, flat(t)))

            @pl.loop(0, 8)
            def _(d):
                for i, (t, o) in enumerate(owners):
                    for h in range(2):
                        w.ss[k, d, j, t[a], h] = plane[i, w.wanted[wi, d, h, o]]

            me = end_index(k, here)
            for i, (t, o) in enumerate(owners):
                for h in range(2):
                    block = plane[i, w.wanted[wi, me, h, o]]
                    tabs[n][t[0], t[1], t[2], t[3], h, SEG * k : SEG * (k + 1), :] = block
            at = list(owners[0][0])
            at[a] = slice(None)
            goal = tabs[n].at[at[0], at[1], at[2], at[3], :, pl.ds(SEG * k, SEG), :]
            for to in ends(k):
                send(w.ss.at[k, end_index(k, to), j], goal, w.sem_us.at[n, k], w.sem_u.at[n, k], to)

    def build(first, count, base):
        @pl.loop(0, SLOTS)
        def _(s):
            recv = receiver_features(w.geo[s])
            for jj in range(first // 2, (first + count) // 2):
                pair = [feats[base + idx[s, 2 * jj + i]] for i in range(2)]
                factors[s, jj] = pair_factors(jnp.concatenate(pair, axis=0), recv)

    def applied(load, s, first, count):
        total = None
        for jj in range(first // 2, (first + count) // 2):
            lhs = jnp.concatenate([load(idx[s, 2 * jj + i]) for i in range(2)], axis=1)
            term = jnp.dot(lhs, factors[s, jj], preferred_element_type=F32)
            total = term if total is None else total + term
        return total

    def near_apply():
        @pl.loop(0, SLOTS)
        def _(s):
            acc[s] = applied(lambda i: near_s[i], s, 0, NEAR)

    def far_apply(n):
        tab = tabs[n]
        r = rows_of((ROWS, V))
        mark = rows_of((2, V)) == n

        def load(i):
            head = tab[i >> 6, (i >> 5) & 1, (i >> 3) & 3, (i >> 1) & 3, i & 1]
            return jnp.concatenate([head, w.tail[i]], axis=0)

        @pl.loop(0, SLOTS)
        def _(s):
            total = acc[s] + applied(load, s, NEAR, FAR)
            a = [alb_ref[i, pl.ds(s, 1), :] for i in range(3)]
            total = total * jnp.where(r < 25, a[0], jnp.where(r < 50, a[1], a[2]))
            w.wide[:, s, :] = total
            if n == 0:
                value = total.astype(BF16)
                near_s[s] = value
                for k in range(3):
                    planes[1][k][0][0, s] = value[SEG * k : SEG * (k + 1)]
            energy = jnp.sum(total * total * area_ref[pl.ds(s, 1), :], axis=0, keepdims=True)
            w.en_all[mine] += jnp.where(mark, energy, 0.0)

    def tails(rows_of_part):
        for k in range(3):
            w.rem_t[:, k, :] = jnp.dot(canonical(k), rows_of_part(k), preferred_element_type=F32)
        w.tail[...] = w.rem_t[...].astype(BF16)

    first_leg_done(0)
    spread(0, 0)

    @pl.loop(0, SLOTS)
    def _(b):
        feats[2 * NDEV + b] = source_features(w.geo[b])

    build(0, NEAR, 2 * NDEV)
    for j in (1, 3, 2):
        spread(0, j)
    for k in range(3):
        wait_for(rg[k].at[pl.ds(0, 7)], w.sem_g.at[0, k])
        order = canonical(k)
        for g, comp in enumerate(GEO[k]):
            rows = rg[k][:, 1 + g].reshape(256, V)
            w.geo_t[:, comp, :] = jnp.dot(order, rows, preferred_element_type=F32)
    tails(lambda k: rg[k][:, 0].reshape(256, V))

    @pl.loop(0, 2 * NDEV)
    def _(b):
        feats[b] = source_features(w.geo_t[b])

    build(NEAR, FAR, 0)
    near_apply()
    for k in range(3):
        wait_for(w.ss.at[k, pl.ds(0, 7)], w.sem_u.at[0, k])
    far_apply(0)

    first_leg([p[0] for p in planes[1]], w.sem_b1s.at[1], w.sem_b1.at[1])
    second_leg(1, 0, 1)
    for k in range(3):
        w.cr[k, 0, 0] = w.wide[72 + k].astype(BF16)
    cr = [w.cr.at[k] for k in range(3)]
    first_leg([c.at[0] for c in cr], w.sem_r1s, w.sem_r1)
    b1_ref[...] = w.wide[:CH].astype(BF16)
    for k in range(3):
        wait_for(w.ss.at[k, pl.ds(0, 7)], w.sem_us.at[0, k])
    first_leg_done(1)
    spread(1, 0)
    for k in range(3):
        wait_for(cr[k].at[0, pl.ds(0, 3)], w.sem_r1.at[k])
    lines_second_leg(cr, w.sem_r2s, w.sem_r2)
    near_apply()
    for k in range(3):
        wait_for(cr[k].at[pl.ds(0, 3)], w.sem_r2.at[k])
        got = jnp.dot(w.sel[k], w.cr[k].reshape(256, V), preferred_element_type=F32).astype(BF16)
        w.sr[k] = got.reshape(8, 32, V)
        me = end_index(k, here)
        w.rr[k, me] = w.sr[k, me]
        for to in ends(k):
            send(w.sr.at[k, end_index(k, to)], w.rr.at[k, me], w.sem_gs.at[1, k], w.sem_g.at[1, k], to)
    for j in (1, 3, 2):
        spread(1, j)
    for k in range(3):
        wait_for(w.rr.at[k, pl.ds(0, 7)], w.sem_g.at[1, k])
    tails(lambda k: w.rr[k].reshape(256, V))
    for k in range(3):
        wait_for(w.ss.at[k, pl.ds(0, 7)], w.sem_u.at[1, k])
    far_apply(1)

    for off in ORDER:
        send(w.en_all.at[mine], w.en_all.at[mine], w.sem_e.at[0], w.sem_e.at[1], shifted(off))
    b2_ref[...] = w.wide[:CH].astype(BF16)
    wait_for(w.en_all.at[pl.ds(0, NDEV - 1)], w.sem_e.at[1])
    en_ref[...] = jnp.sum(w.en_all[...], axis=0)
    wait_for(w.en_all.at[pl.ds(0, NDEV - 1)], w.sem_e.at[0])
    for k in range(3):
        wait_for(w.r1.at[k, pl.ds(0, 7)], w.sem_rs.at[k])
        wait_for(cp[k].at[0, pl.ds(0, 3)], w.sem_c1s.at[k])
        wait_for(cp[k].at[pl.ds(0, 3)], w.sem_c2s.at[k])
        wait_for(cr[k].at[0, pl.ds(0, 3)], w.sem_r1s.at[k])
        wait_for(cr[k].at[pl.ds(0, 3)], w.sem_r2s.at[k])
        wait_for(rg[k].at[pl.ds(0, 7)], w.sem_gs.at[0, k])
        wait_for(w.rr.at[k, pl.ds(0, 7)], w.sem_gs.at[1, k])
        wait_for(w.ss.at[k, pl.ds(0, 7)], w.sem_us.at[1, k])
        for n in range(2):
            wait_for(planes[n][k][0].at[pl.ds(0, 3)], w.sem_b1s.at[n, k])
            for j in (1, 2, 3):
                wait_for(planes[n][k][j], w.sem_b2s.at[n, k])


def scratch_list():
    vm, dma = pltpu.VMEM, pltpu.SemaphoreType.DMA
    out = [
        ("r1", vm((3, 8, 2, V), I32)),
        ("wanted", pltpu.SMEM((3, 8, 2, V), I32)),
        ("near_s", vm((SLOTS, ROWS, V), BF16)),
        ("wide", vm((ROWS, SLOTS, V), F32)),
        ("geo", vm((SLOTS, 8, V), F32)),
        ("sel", vm((3, 256, 256), BF16)),
        ("cr", vm((3, 4, 4, SLOTS, V), BF16)),
        ("sr", vm((3, 8, 32, V), BF16)),
        ("rr", vm((3, 8, 32, V), BF16)),
        ("ss", vm((3, 8, 4, 4, 2, SEG, V), BF16)),
        ("tab_a", vm((4, 2, 4, 4, 2, 3 * SEG, V), BF16)),
        ("tab_b", vm((4, 2, 4, 4, 2, 3 * SEG, V), BF16)),
        ("geo_t", vm((2 * NDEV, 8, V), F32)),
        ("rem_t", vm((2 * NDEV, 8, V), F32)),
        ("tail", vm((2 * NDEV, 8, V), BF16)),
        ("feats", vm((2 * NDEV + SLOTS, 64, V), BF16)),
        ("factors", vm((SLOTS, (NEAR + FAR) // 2, 2 * V, V), BF16)),
        ("acc", vm((SLOTS, ROWS, V), F32)),
        ("en_all", vm((NDEV, 2, V), F32)),
        ("local_sem", dma),
        ("sem_e", dma((2,))),
        ("sem_b2", dma((2, 3, 4))),
    ]
    for k in range(3):
        size = 1 + len(GEO[k])
        out.append((f"cp{k}", vm((4, 4, size, SLOTS, V), BF16)))
        out.append((f"sg{k}", vm((8, size, 32, V), BF16)))
        out.append((f"rg{k}", vm((8, size, 32, V), BF16)))
        for n, j in itertools.product(range(2), range(4)):
            out.append((f"p{n}{k}{j}", vm((4, SLOTS, SEG, V), BF16)))
    for name in ("r", "rs", "c1", "c1s", "c2", "c2s", "r1", "r1s", "r2", "r2s"):
        out.append((f"sem_{name}", dma((3,))))
    for name in ("b1", "b1s", "b2s", "u", "us", "g", "gs"):
        out.append((f"sem_{name}", dma((2, 3))))
    return out


def body(transfer, positions, normals, area, albedo, pairs, home):
    vm = pl.BlockSpec(memory_space=pltpu.VMEM)
    sm = pl.BlockSpec(memory_space=pltpu.SMEM)
    idx, req = pl.pallas_call(
        index_kernel,
        out_shape=(jax.ShapeDtypeStruct((SLOTS, V), I32), jax.ShapeDtypeStruct((2, V), I32)),
        in_specs=[vm, vm],
        out_specs=(vm, vm),
        scratch_shapes=[pltpu.VMEM((SLOTS, V), I32)],
    )(pairs, home.reshape(16, V))
    major = lambda t: jnp.swapaxes(t, 0, 1)
    bounce = jax.ShapeDtypeStruct((CH, SLOTS, V), BF16)
    b1, b2, en = pl.pallas_call(
        main_kernel,
        out_shape=(bounce, bounce, jax.ShapeDtypeStruct((2, V), F32)),
        in_specs=[sm, vm, vm, vm, vm, vm, vm],
        out_specs=(vm, vm, vm),
        scratch_shapes=[shape for _, shape in scratch_list()],
        compiler_params=pltpu.CompilerParams(
            collective_id=0, has_side_effects=True, vmem_limit_bytes=62 * 2**20
        ),
    )(idx, req, major(transfer), major(positions), major(normals), area, major(albedo))
    energies = jnp.sum(en, axis=1) * (1.0 / (NDEV * SLOTS * CH * V))
    return major(b1), major(b2), energies


def solution(mesh):
    finer = Mesh(mesh.devices.reshape(SZ), AX)
    split = [P(AX, *([None] * n)) for n in (2, 2, 2, 1, 2, 1)]
    return jax.shard_map(
        body,
        mesh=finer,
        in_specs=(*split, P()),
        out_specs=(split[0], split[0], P()),
        check_vma=False,
    )
```

```python
import itertools
import types

import jax
import jax.numpy as jnp
import numpy as np
from jax import lax
from jax.experimental import pallas as pl
from jax.experimental.pallas import tpu as pltpu
from jax.sharding import Mesh
from jax.sharding import PartitionSpec as P

AX = ("y", "c", "z", "x")
SZ = (4, 2, 4, 4)
NDEV = 128
SLOTS, NEAR, FAR, CH, V = 16, 16, 24, 75, 128
ROWS = 80
F32, BF16, I32 = jnp.float32, jnp.bfloat16, jnp.int32
MESH = pl.DeviceIdType.MESH


def rounded(t):
    return t.astype(BF16).astype(F32)


def pieces3(t):
    a = rounded(t)
    b = rounded(t - a)
    return a, b, rounded(t - a - b)


def rows_of(shape):
    return lax.broadcasted_iota(I32, shape, 0)


def source_features(v):
    r = rows_of((8, V))
    vh = rounded(v)
    vl = rounded(v - vh)
    m = -(v * v[6:7])
    mh = rounded(m)
    ml = rounded(m - mh)
    x = jnp.where(r < 3, v, 0.0)
    c = pieces3(jnp.sum(pltpu.roll(m, 5, 0) * x, axis=0, keepdims=True))
    e = pieces3(jnp.sum(x * x, axis=0, keepdims=True) + 1.0)
    cv = jnp.ones((8, V), F32)
    for i, row in enumerate(c + e):
        cv = jnp.where(r == i, row, cv)
    return jnp.concatenate([vh, vh, vl, mh, mh, ml, cv, jnp.zeros((8, V), F32)], axis=0).astype(BF16)


def receiver_features(v):
    r = rows_of((8, V))
    z = jnp.zeros((8, V), F32)
    x = jnp.where(r < 3, v, 0.0)
    n = jnp.where(r < 3, pltpu.roll(v, 5, 0), 0.0) * (1.0 / np.pi)
    nh = rounded(n)
    nl = rounded(n - nh)
    xh = rounded(x)
    xl = rounded(x - xh)
    k = pieces3(-jnp.sum(n * x, axis=0, keepdims=True))
    q = pieces3(jnp.sum(x * x, axis=0, keepdims=True))
    xh3 = -pltpu.roll(xh, 3, 0)
    xl3 = -pltpu.roll(xl, 3, 0)
    last = r == 7
    ap = [jnp.where(last, k[0], nh), jnp.where(last, k[1], nl), nh, z, z, z, jnp.where(r == 6, k[2], z), z]
    aq = [z, z, z, xh3, xl3, xh3, jnp.where(r < 3, 1.0, z), z]
    d = [jnp.where(last, q[0], -2.0 * xh), jnp.where(last, q[1], -2.0 * xl), -2.0 * xh, z, z, z,
         jnp.where((r >= 3) & (r < 6), 1.0, jnp.where(r == 6, q[2], z)), z]
    ap, aq, d = (jnp.concatenate(t, axis=0).astype(BF16) for t in (ap, aq, d))
    o = jnp.zeros((64, V), BF16)
    top = jnp.concatenate([ap, aq, o, o, d, o], axis=1)
    bottom = jnp.concatenate([o, o, ap, aq, o, d], axis=1)
    return jnp.concatenate([top, bottom], axis=0)


def pair_factors(feats, recv):
    out = lax.dot_general(feats, recv, (((0,), (0,)), ((), ())), preferred_element_type=F32)
    parts = []
    for i in range(2):
        ap = out[:, 256 * i : 256 * i + 128]
        aq = out[:, 256 * i + 128 : 256 * i + 256]
        d = out[:, 512 + 128 * i : 640 + 128 * i]
        parts.append((jnp.maximum(ap, 0.0) * jnp.maximum(aq, 0.0) / (d * d)).astype(BF16))
    return jnp.concatenate(parts, axis=0)


def me4():
    return tuple(lax.axis_index(a) for a in AX)


def my_index():
    y, c, z, x = me4()
    return ((y * 2 + c) * 4 + z) * 4 + x


def shifted(off):
    return tuple(lax.rem(i + o, s) for i, o, s in zip(me4(), off, SZ))


def flat(t):
    return ((t[0] * 2 + t[1]) * 4 + t[2]) * 4 + t[3]


def index_kernel(pairs_ref, home_ref, idx_ref, req_ref, wide_ref):
    wide_ref[...] = jnp.zeros((SLOTS, V), I32)
    wide_ref[:, : NEAR + FAR] = pairs_ref[...]
    p = wide_ref[...]
    home = home_ref[...]
    shape = (SLOTS, V)
    lane = lax.broadcasted_iota(I32, shape, 1)
    low, high = p & 127, p >> 7
    slot = jnp.zeros(shape, I32)
    for h in range(16):
        got = jnp.take_along_axis(jnp.broadcast_to(home[h : h + 1], shape), low, axis=1)
        slot = jnp.where(high == h, got, slot)
    owner, local = slot >> 4, slot & 15
    lo = jnp.full(shape, 99, I32)
    hi = jnp.full(shape, -1, I32)
    for j in range(NEAR, NEAR + FAR):
        same = owner[:, j : j + 1] == lane
        lo = jnp.where(same, jnp.minimum(lo, local[:, j : j + 1]), lo)
        hi = jnp.where(same, jnp.maximum(hi, local[:, j : j + 1]), hi)
    lo = jnp.min(lo, axis=0, keepdims=True)
    hi = jnp.max(hi, axis=0, keepdims=True)
    lo = jnp.where(lo > 15, 0, lo)
    hi = jnp.where(hi < 0, 0, hi)
    first = jnp.take_along_axis(jnp.broadcast_to(lo, shape), owner, axis=1)
    far = owner * 2 + jnp.where(local != first, 1, 0)
    idx_ref[...] = jnp.where(lane < NEAR, local, far)
    req_ref[...] = jnp.where(rows_of((2, V)) == 0, lo, hi)


OFFSETS = [o for o in itertools.product(range(4), range(2), range(4), range(4)) if any(o)]
ORDER = [OFFSETS[i] for i in np.random.RandomState(0).permutation(len(OFFSETS))]

DIMS = (0, 2, 3)
AXES = ((0, 2, 3), (2, 3, 0), (3, 0, 2))
STEPS = (2, 1, 3)
SEG = 24
GEO = ((0, 1, 2), (3, 4), (5, 6))
FROM = (0, 3, 2, 1)


def moved(dim, by, core=0):
    off = [0, core, 0, 0]
    off[dim] = by
    return tuple(off)


def send(src, dst, send_sem, recv_sem, to):
    pltpu.make_async_remote_copy(
        src, dst, send_sem, recv_sem, device_id=to, device_id_type=MESH
    ).start()


def wait_for(part, sem):
    pltpu.make_async_copy(part, part, sem).wait()


def row_column(shape):
    return rows_of(shape), lax.broadcasted_iota(I32, shape, 1)


def selection(k, table):
    here = me4()
    a, b, _ = AXES[k]
    r, m = row_column((256, 16))
    expand = jnp.where(m == ((r >> 5) << 1) + (r & 1), 1.0, 0.0).astype(BF16)
    wide = jnp.dot(expand, table.astype(F32).astype(BF16), preferred_element_type=F32)
    r, lane = row_column((256, V))
    coords = list(here)
    coords[a] = (here[a] + ((r >> 1) & 3)) & 3
    coords[b] = (here[b] + ((r >> 3) & 3)) & 3
    value = jnp.sum(jnp.where(lane == flat(coords), wide, 0.0), axis=1, keepdims=True)
    r, lane = row_column((256, 256))
    place = (lane - (((r >> 1) & 15) << 4)).astype(F32)
    return jnp.where(value == place, 1.0, 0.0).astype(BF16)


def canonical(k):
    here = me4()
    a, b, c = AXES[k]
    r, col = row_column((256, 256))
    t = (r >> 6, (r >> 5) & 1, (r >> 3) & 3, (r >> 1) & 3)
    i = (t[a] - here[a]) & 3
    j = (t[b] - here[b]) & 3
    place = (((t[c] << 1) + t[1]) << 5) + (j << 3) + (i << 1) + (r & 1)
    return jnp.where(place == col, 1.0, 0.0).astype(BF16)


def main_kernel(idx, req_ref, tr_ref, pos_ref, nrm_ref, area_ref, alb_ref, b1_ref, b2_ref, en_ref, *scratch):
    w = types.SimpleNamespace(**dict(zip([n for n, _ in scratch_list()], scratch)))
    factors, feats, acc, near_s = w.factors, w.feats, w.acc, w.near_s
    cp, sg, rg = (w.cp0, w.cp1, w.cp2), (w.sg0, w.sg1, w.sg2), (w.rg0, w.rg1, w.rg2)
    planes = [[[getattr(w, f"p{n}{k}{j}") for j in range(4)] for k in range(3)] for n in range(2)]
    tabs = (w.tab_a, w.tab_b)
    here = me4()
    core = here[1]
    mine = my_index()
    partner = shifted((0, 1, 0, 0))
    line = {d: {by: shifted(moved(d, by)) for by in STEPS} for d in DIMS}
    other = {d: {by: shifted(moved(d, by, 1)) for by in STEPS} for d in DIMS}

    barrier = pltpu.get_barrier_semaphore()
    greeted = [partner] + [t[d][by] for t in (line, other) for d in DIMS for by in STEPS]
    for to in greeted:
        pl.semaphore_signal(barrier, inc=1, device_id=to, device_id_type=MESH)

    for i in range(3):
        w.r1[i, here[DIMS[i]] * 2 + core] = req_ref[...]
    w.wide[:CH] = tr_ref[...].astype(F32)
    w.wide[CH:] = jnp.zeros((ROWS - CH, SLOTS, V), F32)
    comps = [pos_ref.at[0], pos_ref.at[1], pos_ref.at[2], nrm_ref.at[0], nrm_ref.at[1], nrm_ref.at[2], area_ref]
    for i, comp in enumerate(comps):
        w.geo[:, i, :] = comp[...]
    w.geo[:, 7, :] = jnp.ones((SLOTS, V), F32)
    for s in range(SLOTS):
        value = w.wide[:, s, :].astype(BF16)
        near_s[s] = value
        for k in range(3):
            planes[0][k][0][0, s] = value[SEG * k : SEG * (k + 1)]
    for k in range(3):
        cp[k][0, 0, 0] = tr_ref[72 + k]
        for g, comp in enumerate(GEO[k]):
            cp[k][0, 0, 1 + g] = comps[comp][...].astype(BF16)
    pl.semaphore_wait(barrier, len(greeted))

    for i in range(3):
        slot = w.r1.at[i, here[DIMS[i]] * 2 + core]
        for to in [line[DIMS[i]][by] for by in STEPS] + [other[DIMS[i]][by] for by in STEPS] + [partner]:
            send(req_ref, slot, w.sem_rs.at[i], w.sem_r.at[i], to)

    def first_leg(refs, send_sem, recv_sem):
        for by in STEPS:
            for k in range(3):
                send(refs[k].at[0], refs[k].at[FROM[by]], send_sem.at[k], recv_sem.at[k], line[AXES[k][0]][by])

    first_leg([c.at[0] for c in cp], w.sem_c1s, w.sem_c1)
    first_leg([p[0] for p in planes[0]], w.sem_b1s.at[0], w.sem_b1.at[0])

    def build(first, count, base, start, stop):
        @pl.loop(start, stop)
        def _(s):
            recv = receiver_features(w.geo[s])
            for jj in range(first // 2, (first + count) // 2):
                pair = [feats[base + idx[s, 2 * jj + i]] for i in range(2)]
                factors[s, jj] = pair_factors(jnp.concatenate(pair, axis=0), recv)

    def second_leg(n, part, size):
        for by in STEPS:
            for k in range(3):
                send(planes[n][k][0].at[pl.ds(part, size)], planes[n][k][FROM[by]].at[pl.ds(part, size)],
                     w.sem_b2s.at[n, k], w.sem_b2.at[n, k, FROM[by]], line[AXES[k][1]][by])

    def first_leg_done(n):
        for k in range(3):
            wait_for(planes[n][k][0].at[pl.ds(0, 3)], w.sem_b1.at[n, k])

    def lines_second_leg(refs, send_sem, recv_sem):
        for by in STEPS:
            for k in range(3):
                send(refs[k].at[0], refs[k].at[FROM[by]], send_sem.at[k], recv_sem.at[k], line[AXES[k][1]][by])

    @pl.loop(0, SLOTS)
    def _(b):
        feats[2 * NDEV + b] = source_features(w.geo[b])

    build(0, NEAR, 2 * NDEV, 0, 8)
    for k in range(3):
        wait_for(cp[k].at[0, pl.ds(0, 3)], w.sem_c1.at[k])
    lines_second_leg(cp, w.sem_c2s, w.sem_c2)
    second_leg(0, 0, 1)

    w.rem_t[...] = jnp.zeros((2 * NDEV, 8, V), F32)
    w.geo_t[:, 7, :] = jnp.ones((2 * NDEV, V), F32)
    w.en_all[mine] = jnp.zeros((2, V), F32)
    for i in range(3):
        wait_for(w.r1.at[i, pl.ds(0, 7)], w.sem_r.at[i])
    copy = pltpu.make_async_copy(w.r1, w.wanted, w.local_sem)
    copy.start()
    for k in range(3):
        i = DIMS.index(AXES[k][2])
        w.sel[k] = selection(k, jnp.concatenate([w.r1[i, d] for d in range(8)], axis=0))

    build(0, NEAR, 2 * NDEV, 8, 12)
    first_leg_done(0)
    second_leg(0, 1, 1)
    build(0, NEAR, 2 * NDEV, 12, SLOTS)

    def ends(k):
        c = AXES[k][2]
        return [shifted(moved(c, by, o)) for by, o in ((2, 0), (2, 1), (1, 0), (1, 1), (3, 0), (3, 1), (0, 1))]

    def end_index(k, t):
        return t[AXES[k][2]] * 2 + t[1]

    for k in range(3):
        wait_for(cp[k].at[pl.ds(0, 3)], w.sem_c2.at[k])
        for g in range(1 + len(GEO[k])):
            source = cp[k][:, :, g].reshape(256, V)
            got = jnp.dot(w.sel[k], source, preferred_element_type=F32).astype(BF16)
            sg[k][:, g] = got.reshape(8, 32, V)
        me = end_index(k, here)
        rg[k][me] = sg[k][me]
        for to in ends(k):
            send(sg[k].at[end_index(k, to)], rg[k].at[me], w.sem_gs.at[0, k], w.sem_g.at[0, k], to)

    def spread(n, j):
        for k in range(3):
            a, b, c = AXES[k]
            wi = DIMS.index(c)
            plane = planes[n][k][j]
            if j:
                wait_for(plane, w.sem_b2.at[n, k, j])
            owners = []
            for i in range(4):
                t = list(here)
                t[a] = (here[a] + i) & 3
                t[b] = (here[b] + j) & 3
                owners.append((t, flat(t)))

            @pl.loop(0, 8)
            def _(d):
                for i, (t, o) in enumerate(owners):
                    for h in range(2):
                        w.ss[k, d, j, t[a], h] = plane[i, w.wanted[wi, d, h, o]]

            me = end_index(k, here)
            for i, (t, o) in enumerate(owners):
                for h in range(2):
                    block = plane[i, w.wanted[wi, me, h, o]]
                    tabs[n][t[0], t[1], t[2], t[3], h, SEG * k : SEG * (k + 1), :] = block
            at = list(owners[0][0])
            at[a] = slice(None)
            goal = tabs[n].at[at[0], at[1], at[2], at[3], :, pl.ds(SEG * k, SEG), :]
            for to in ends(k):
                send(w.ss.at[k, end_index(k, to), j], goal, w.sem_us.at[n, k], w.sem_u.at[n, k], to)

    def applied(load, s, first, count):
        total = None
        for jj in range(first // 2, (first + count) // 2):
            lhs = jnp.concatenate([load(idx[s, 2 * jj + i]) for i in range(2)], axis=1)
            term = jnp.dot(lhs, factors[s, jj], preferred_element_type=F32)
            total = term if total is None else total + term
        return total

    def near_apply():
        @pl.loop(0, SLOTS)
        def _(s):
            acc[s] = applied(lambda i: near_s[i], s, 0, NEAR)

    def far_apply(n, start, stop):
        tab = tabs[n]
        r = rows_of((ROWS, V))
        mark = rows_of((2, V)) == n

        def load(i):
            head = tab[i >> 6, (i >> 5) & 1, (i >> 3) & 3, (i >> 1) & 3, i & 1]
            return jnp.concatenate([head, w.tail[i]], axis=0)

        @pl.loop(start, stop)
        def _(s):
            total = acc[s] + applied(load, s, NEAR, FAR)
            a = [alb_ref[i, pl.ds(s, 1), :] for i in range(3)]
            total = total * jnp.where(r < 25, a[0], jnp.where(r < 50, a[1], a[2]))
            w.wide[:, s, :] = total
            if n == 0:
                value = total.astype(BF16)
                near_s[s] = value
                for k in range(3):
                    planes[1][k][0][0, s] = value[SEG * k : SEG * (k + 1)]
            energy = jnp.sum(total * total * area_ref[pl.ds(s, 1), :], axis=0, keepdims=True)
            w.en_all[mine] += jnp.where(mark, energy, 0.0)

    def tails(rows_of_part):
        for k in range(3):
            w.rem_t[:, k, :] = jnp.dot(canonical(k), rows_of_part(k), preferred_element_type=F32)
        w.tail[...] = w.rem_t[...].astype(BF16)

    second_leg(0, 2, 2)
    copy.wait()
    spread(0, 0)
    for k in range(3):
        wait_for(rg[k].at[pl.ds(0, 7)], w.sem_g.at[0, k])
        order = canonical(k)
        for g, comp in enumerate(GEO[k]):
            rows = rg[k][:, 1 + g].reshape(256, V)
            w.geo_t[:, comp, :] = jnp.dot(order, rows, preferred_element_type=F32)
    tails(lambda k: rg[k][:, 0].reshape(256, V))

    @pl.loop(0, 2 * NDEV)
    def _(b):
        feats[b] = source_features(w.geo_t[b])

    build(NEAR, FAR, 0, 0, 6)
    for j in (1, 3, 2):
        spread(0, j)
    build(NEAR, FAR, 0, 6, SLOTS)
    near_apply()
    for k in range(3):
        wait_for(w.ss.at[k, pl.ds(0, 7)], w.sem_u.at[0, k])

    def half_leg(start):
        part = pl.ds(start, SLOTS // 2)
        for by in STEPS:
            for k in range(3):
                line0 = planes[1][k][0]
                send(line0.at[0, part], line0.at[FROM[by], part],
                     w.sem_b1s.at[1, k], w.sem_b1.at[1, k], line[AXES[k][0]][by])

    far_apply(0, 0, SLOTS // 2)
    half_leg(0)
    far_apply(0, SLOTS // 2, SLOTS)
    for k in range(3):
        w.cr[k, 0, 0] = w.wide[72 + k].astype(BF16)
    cr = [w.cr.at[k] for k in range(3)]
    first_leg([c.at[0] for c in cr], w.sem_r1s, w.sem_r1)
    half_leg(SLOTS // 2)
    second_leg(1, 0, 1)
    b1_ref[...] = w.wide[:CH].astype(BF16)
    for k in range(3):
        wait_for(w.ss.at[k, pl.ds(0, 7)], w.sem_us.at[0, k])
    for k in range(3):
        wait_for(cr[k].at[0, pl.ds(0, 3)], w.sem_r1.at[k])
    lines_second_leg(cr, w.sem_r2s, w.sem_r2)
    first_leg_done(1)
    second_leg(1, 1, 3)
    spread(1, 0)
    near_apply()
    for k in range(3):
        wait_for(cr[k].at[pl.ds(0, 3)], w.sem_r2.at[k])
        got = jnp.dot(w.sel[k], w.cr[k].reshape(256, V), preferred_element_type=F32).astype(BF16)
        w.sr[k] = got.reshape(8, 32, V)
        me = end_index(k, here)
        w.rr[k, me] = w.sr[k, me]
        for to in ends(k):
            send(w.sr.at[k, end_index(k, to)], w.rr.at[k, me], w.sem_gs.at[1, k], w.sem_g.at[1, k], to)
    for j in (1, 3, 2):
        spread(1, j)
    for k in range(3):
        wait_for(w.rr.at[k, pl.ds(0, 7)], w.sem_g.at[1, k])
    tails(lambda k: w.rr[k].reshape(256, V))
    for k in range(3):
        wait_for(w.ss.at[k, pl.ds(0, 7)], w.sem_u.at[1, k])
    far_apply(1, 0, SLOTS)

    for off in ORDER:
        send(w.en_all.at[mine], w.en_all.at[mine], w.sem_e.at[0], w.sem_e.at[1], shifted(off))
    b2_ref[...] = w.wide[:CH].astype(BF16)
    wait_for(w.en_all.at[pl.ds(0, NDEV - 1)], w.sem_e.at[1])
    en_ref[...] = jnp.sum(w.en_all[...], axis=0)
    wait_for(w.en_all.at[pl.ds(0, NDEV - 1)], w.sem_e.at[0])
    for k in range(3):
        wait_for(w.r1.at[k, pl.ds(0, 7)], w.sem_rs.at[k])
        wait_for(cp[k].at[0, pl.ds(0, 3)], w.sem_c1s.at[k])
        wait_for(cp[k].at[pl.ds(0, 3)], w.sem_c2s.at[k])
        wait_for(cr[k].at[0, pl.ds(0, 3)], w.sem_r1s.at[k])
        wait_for(cr[k].at[pl.ds(0, 3)], w.sem_r2s.at[k])
        wait_for(rg[k].at[pl.ds(0, 7)], w.sem_gs.at[0, k])
        wait_for(w.rr.at[k, pl.ds(0, 7)], w.sem_gs.at[1, k])
        wait_for(w.ss.at[k, pl.ds(0, 7)], w.sem_us.at[1, k])
        for n in range(2):
            wait_for(planes[n][k][0].at[pl.ds(0, 3)], w.sem_b1s.at[n, k])
            for j in (1, 2, 3):
                wait_for(planes[n][k][j], w.sem_b2s.at[n, k])


def last_kernel(b1_ref, b2_ref, en_ref, o1_ref, o2_ref, sum_ref):
    o1_ref[...] = b1_ref[...]
    o2_ref[...] = b2_ref[...]
    for i in range(2):
        sum_ref[i] = jnp.sum(en_ref[i : i + 1, :]) * (1.0 / (NDEV * SLOTS * CH * V))


def scratch_list():
    vm, dma = pltpu.VMEM, pltpu.SemaphoreType.DMA
    out = [
        ("r1", vm((3, 8, 2, V), I32)),
        ("wanted", pltpu.SMEM((3, 8, 2, V), I32)),
        ("near_s", vm((SLOTS, ROWS, V), BF16)),
        ("wide", vm((ROWS, SLOTS, V), F32)),
        ("geo", vm((SLOTS, 8, V), F32)),
        ("sel", vm((3, 256, 256), BF16)),
        ("cr", vm((3, 4, 4, SLOTS, V), BF16)),
        ("sr", vm((3, 8, 32, V), BF16)),
        ("rr", vm((3, 8, 32, V), BF16)),
        ("ss", vm((3, 8, 4, 4, 2, SEG, V), BF16)),
        ("tab_a", vm((4, 2, 4, 4, 2, 3 * SEG, V), BF16)),
        ("tab_b", vm((4, 2, 4, 4, 2, 3 * SEG, V), BF16)),
        ("geo_t", vm((2 * NDEV, 8, V), F32)),
        ("rem_t", vm((2 * NDEV, 8, V), F32)),
        ("tail", vm((2 * NDEV, 8, V), BF16)),
        ("feats", vm((2 * NDEV + SLOTS, 64, V), BF16)),
        ("factors", vm((SLOTS, (NEAR + FAR) // 2, 2 * V, V), BF16)),
        ("acc", vm((SLOTS, ROWS, V), F32)),
        ("en_all", vm((NDEV, 2, V), F32)),
        ("local_sem", dma),
        ("sem_e", dma((2,))),
        ("sem_b2", dma((2, 3, 4))),
    ]
    for k in range(3):
        size = 1 + len(GEO[k])
        out.append((f"cp{k}", vm((4, 4, size, SLOTS, V), BF16)))
        out.append((f"sg{k}", vm((8, size, 32, V), BF16)))
        out.append((f"rg{k}", vm((8, size, 32, V), BF16)))
        for n, j in itertools.product(range(2), range(4)):
            out.append((f"p{n}{k}{j}", vm((4, SLOTS, SEG, V), BF16)))
    for name in ("r", "rs", "c1", "c1s", "c2", "c2s", "r1", "r1s", "r2", "r2s"):
        out.append((f"sem_{name}", dma((3,))))
    for name in ("b1", "b1s", "b2s", "u", "us", "g", "gs"):
        out.append((f"sem_{name}", dma((2, 3))))
    return out


def body(transfer, positions, normals, area, albedo, pairs, home):
    vm = pl.BlockSpec(memory_space=pltpu.VMEM)
    sm = pl.BlockSpec(memory_space=pltpu.SMEM)
    idx, req = pl.pallas_call(
        index_kernel,
        out_shape=(jax.ShapeDtypeStruct((SLOTS, V), I32), jax.ShapeDtypeStruct((2, V), I32)),
        in_specs=[vm, vm],
        out_specs=(vm, vm),
        scratch_shapes=[pltpu.VMEM((SLOTS, V), I32)],
    )(pairs, home.reshape(16, V))
    major = lambda t: jnp.swapaxes(t, 0, 1)
    bounce = jax.ShapeDtypeStruct((CH, SLOTS, V), BF16)
    b1, b2, en = pl.pallas_call(
        main_kernel,
        out_shape=(bounce, bounce, jax.ShapeDtypeStruct((2, V), F32)),
        in_specs=[sm, vm, vm, vm, vm, vm, vm],
        out_specs=(vm, vm, vm),
        scratch_shapes=[shape for _, shape in scratch_list()],
        compiler_params=pltpu.CompilerParams(
            collective_id=0, has_side_effects=True, vmem_limit_bytes=62 * 2**20
        ),
    )(idx, req, major(transfer), major(positions), major(normals), area, major(albedo))
    b1, b2, energies = pl.pallas_call(
        last_kernel,
        out_shape=(bounce, bounce, jax.ShapeDtypeStruct((2,), F32)),
        in_specs=[vm, vm, vm],
        out_specs=(vm, vm, sm),
    )(b1, b2, en)
    return major(b1), major(b2), energies


def solution(mesh):
    finer = Mesh(mesh.devices.reshape(SZ), AX)
    split = [P(AX, *([None] * n)) for n in (2, 2, 2, 1, 2, 1)]
    return jax.shard_map(
        body,
        mesh=finer,
        in_specs=(*split, P()),
        out_specs=(split[0], split[0], P()),
        check_vma=False,
    )
```

```python
import itertools
import types

import jax
import jax.numpy as jnp
import numpy as np
from jax import lax
from jax.experimental import pallas as pl
from jax.experimental.pallas import tpu as pltpu
from jax.sharding import Mesh
from jax.sharding import PartitionSpec as P

AX = ("y", "c", "z", "x")
SZ = (4, 2, 4, 4)
NDEV = 128
SLOTS, NEAR, FAR, CH, V = 16, 16, 24, 75, 128
ROWS = 80
F32, BF16, I32 = jnp.float32, jnp.bfloat16, jnp.int32
MESH = pl.DeviceIdType.MESH


def rounded(t):
    return t.astype(BF16).astype(F32)


def pieces3(t):
    a = rounded(t)
    b = rounded(t - a)
    return a, b, rounded(t - a - b)


def rows_of(shape):
    return lax.broadcasted_iota(I32, shape, 0)


def source_features(v):
    r = rows_of((8, V))
    vh = rounded(v)
    vl = rounded(v - vh)
    m = -(v * v[6:7])
    mh = rounded(m)
    ml = rounded(m - mh)
    x = jnp.where(r < 3, v, 0.0)
    c = pieces3(jnp.sum(pltpu.roll(m, 5, 0) * x, axis=0, keepdims=True))
    e = pieces3(jnp.sum(x * x, axis=0, keepdims=True) + 1.0)
    cv = jnp.ones((8, V), F32)
    for i, row in enumerate(c + e):
        cv = jnp.where(r == i, row, cv)
    return jnp.concatenate([vh, vh, vl, mh, mh, ml, cv, jnp.zeros((8, V), F32)], axis=0).astype(BF16)


def receiver_features(v):
    r = rows_of((8, V))
    z = jnp.zeros((8, V), F32)
    x = jnp.where(r < 3, v, 0.0)
    n = jnp.where(r < 3, pltpu.roll(v, 5, 0), 0.0) * (1.0 / np.pi)
    nh = rounded(n)
    nl = rounded(n - nh)
    xh = rounded(x)
    xl = rounded(x - xh)
    k = pieces3(-jnp.sum(n * x, axis=0, keepdims=True))
    q = pieces3(jnp.sum(x * x, axis=0, keepdims=True))
    xh3 = -pltpu.roll(xh, 3, 0)
    xl3 = -pltpu.roll(xl, 3, 0)
    last = r == 7
    ap = [jnp.where(last, k[0], nh), jnp.where(last, k[1], nl), nh, z, z, z, jnp.where(r == 6, k[2], z), z]
    aq = [z, z, z, xh3, xl3, xh3, jnp.where(r < 3, 1.0, z), z]
    d = [jnp.where(last, q[0], -2.0 * xh), jnp.where(last, q[1], -2.0 * xl), -2.0 * xh, z, z, z,
         jnp.where((r >= 3) & (r < 6), 1.0, jnp.where(r == 6, q[2], z)), z]
    ap, aq, d = (jnp.concatenate(t, axis=0).astype(BF16) for t in (ap, aq, d))
    o = jnp.zeros((64, V), BF16)
    top = jnp.concatenate([ap, aq, o, o, d, o], axis=1)
    bottom = jnp.concatenate([o, o, ap, aq, o, d], axis=1)
    return jnp.concatenate([top, bottom], axis=0)


def pair_factors(feats, recv):
    out = lax.dot_general(feats, recv, (((0,), (0,)), ((), ())), preferred_element_type=F32)
    parts = []
    for i in range(2):
        ap = out[:, 256 * i : 256 * i + 128]
        aq = out[:, 256 * i + 128 : 256 * i + 256]
        d = out[:, 512 + 128 * i : 640 + 128 * i]
        parts.append((jnp.maximum(ap, 0.0) * jnp.maximum(aq, 0.0) / (d * d)).astype(BF16))
    return jnp.concatenate(parts, axis=0)


def me4():
    return tuple(lax.axis_index(a) for a in AX)


def my_index():
    y, c, z, x = me4()
    return ((y * 2 + c) * 4 + z) * 4 + x


def shifted(off):
    return tuple(lax.rem(i + o, s) for i, o, s in zip(me4(), off, SZ))


def flat(t):
    return ((t[0] * 2 + t[1]) * 4 + t[2]) * 4 + t[3]


def index_kernel(pairs_ref, home_ref, idx_ref, req_ref, wide_ref):
    wide_ref[...] = jnp.zeros((SLOTS, V), I32)
    wide_ref[:, : NEAR + FAR] = pairs_ref[...]
    p = wide_ref[...]
    home = home_ref[...]
    shape = (SLOTS, V)
    lane = lax.broadcasted_iota(I32, shape, 1)
    low, high = p & 127, p >> 7
    slot = jnp.zeros(shape, I32)
    for h in range(16):
        got = jnp.take_along_axis(jnp.broadcast_to(home[h : h + 1], shape), low, axis=1)
        slot = jnp.where(high == h, got, slot)
    owner, local = slot >> 4, slot & 15
    lo = jnp.full(shape, 99, I32)
    hi = jnp.full(shape, -1, I32)
    for j in range(NEAR, NEAR + FAR):
        same = owner[:, j : j + 1] == lane
        lo = jnp.where(same, jnp.minimum(lo, local[:, j : j + 1]), lo)
        hi = jnp.where(same, jnp.maximum(hi, local[:, j : j + 1]), hi)
    lo = jnp.min(lo, axis=0, keepdims=True)
    hi = jnp.max(hi, axis=0, keepdims=True)
    lo = jnp.where(lo > 15, 0, lo)
    hi = jnp.where(hi < 0, 0, hi)
    first = jnp.take_along_axis(jnp.broadcast_to(lo, shape), owner, axis=1)
    far = owner * 2 + jnp.where(local != first, 1, 0)
    idx_ref[...] = jnp.where(lane < NEAR, local, far)
    req_ref[...] = jnp.where(rows_of((2, V)) == 0, lo, hi)


OFFSETS = [o for o in itertools.product(range(4), range(2), range(4), range(4)) if any(o)]
ORDER = [OFFSETS[i] for i in np.random.RandomState(0).permutation(len(OFFSETS))]

DIMS = (0, 2, 3)
AXES = ((0, 2, 3), (2, 3, 0), (3, 0, 2))
STEPS = (2, 1, 3)
SEG = 24
GEO = ((0, 1, 2), (3, 4), (5, 6))
FROM = (0, 3, 2, 1)


def moved(dim, by, core=0):
    off = [0, core, 0, 0]
    off[dim] = by
    return tuple(off)


def send(src, dst, send_sem, recv_sem, to):
    pltpu.make_async_remote_copy(
        src, dst, send_sem, recv_sem, device_id=to, device_id_type=MESH
    ).start()


def wait_for(part, sem):
    pltpu.make_async_copy(part, part, sem).wait()


def row_column(shape):
    return rows_of(shape), lax.broadcasted_iota(I32, shape, 1)


def selection(k, table):
    here = me4()
    a, b, _ = AXES[k]
    r, m = row_column((256, 16))
    expand = jnp.where(m == ((r >> 5) << 1) + (r & 1), 1.0, 0.0).astype(BF16)
    wide = jnp.dot(expand, table.astype(F32).astype(BF16), preferred_element_type=F32)
    r, lane = row_column((256, V))
    coords = list(here)
    coords[a] = (here[a] + ((r >> 1) & 3)) & 3
    coords[b] = (here[b] + ((r >> 3) & 3)) & 3
    value = jnp.sum(jnp.where(lane == flat(coords), wide, 0.0), axis=1, keepdims=True)
    r, lane = row_column((256, 256))
    place = (lane - (((r >> 1) & 15) << 4)).astype(F32)
    return jnp.where(value == place, 1.0, 0.0).astype(BF16)


def canonical(k):
    here = me4()
    a, b, c = AXES[k]
    r, col = row_column((256, 256))
    t = (r >> 6, (r >> 5) & 1, (r >> 3) & 3, (r >> 1) & 3)
    i = (t[a] - here[a]) & 3
    j = (t[b] - here[b]) & 3
    place = (((t[c] << 1) + t[1]) << 5) + (j << 3) + (i << 1) + (r & 1)
    return jnp.where(place == col, 1.0, 0.0).astype(BF16)


def main_kernel(idx, req_ref, tr_ref, pos_ref, nrm_ref, area_ref, alb_ref, b1_ref, b2_ref, en_ref, *scratch):
    w = types.SimpleNamespace(**dict(zip([n for n, _ in scratch_list()], scratch)))
    factors, feats, acc, near_s = w.factors, w.feats, w.acc, w.near_s
    cp, sg, rg = (w.cp0, w.cp1, w.cp2), (w.sg0, w.sg1, w.sg2), (w.rg0, w.rg1, w.rg2)
    planes = [[[getattr(w, f"p{n}{k}{j}") for j in range(4)] for k in range(3)] for n in range(2)]
    tabs = (w.tab_a, w.tab_b)
    here = me4()
    core = here[1]
    mine = my_index()
    partner = shifted((0, 1, 0, 0))
    line = {d: {by: shifted(moved(d, by)) for by in STEPS} for d in DIMS}
    other = {d: {by: shifted(moved(d, by, 1)) for by in STEPS} for d in DIMS}

    barrier = pltpu.get_barrier_semaphore()
    greeted = [partner] + [t[d][by] for t in (line, other) for d in DIMS for by in STEPS]
    for to in greeted:
        pl.semaphore_signal(barrier, inc=1, device_id=to, device_id_type=MESH)

    for i in range(3):
        w.r1[i, here[DIMS[i]] * 2 + core] = req_ref[...]
    w.wide[:CH] = tr_ref[...].astype(F32)
    w.wide[CH:] = jnp.zeros((ROWS - CH, SLOTS, V), F32)
    comps = [pos_ref.at[0], pos_ref.at[1], pos_ref.at[2], nrm_ref.at[0], nrm_ref.at[1], nrm_ref.at[2], area_ref]
    for i, comp in enumerate(comps):
        w.geo[:, i, :] = comp[...]
    w.geo[:, 7, :] = jnp.ones((SLOTS, V), F32)
    for s in range(SLOTS):
        value = w.wide[:, s, :].astype(BF16)
        near_s[s] = value
        for k in range(3):
            planes[0][k][0][0, s] = value[SEG * k : SEG * (k + 1)]
    for k in range(3):
        cp[k][0, 0, 0] = tr_ref[72 + k]
        for g, comp in enumerate(GEO[k]):
            cp[k][0, 0, 1 + g] = comps[comp][...].astype(BF16)
    pl.semaphore_wait(barrier, len(greeted))

    for i in range(3):
        slot = w.r1.at[i, here[DIMS[i]] * 2 + core]
        for to in [line[DIMS[i]][by] for by in STEPS] + [other[DIMS[i]][by] for by in STEPS] + [partner]:
            send(req_ref, slot, w.sem_rs.at[i], w.sem_r.at[i], to)

    def first_leg(refs, send_sem, recv_sem):
        for by in STEPS:
            for k in range(3):
                send(refs[k].at[0], refs[k].at[FROM[by]], send_sem.at[k], recv_sem.at[k], line[AXES[k][0]][by])

    first_leg([c.at[0] for c in cp], w.sem_c1s, w.sem_c1)
    first_leg([p[0] for p in planes[0]], w.sem_b1s.at[0], w.sem_b1.at[0])

    def build(first, count, base, start, stop):
        @pl.loop(start, stop)
        def _(s):
            recv = receiver_features(w.geo[s])
            for jj in range(first // 2, (first + count) // 2):
                pair = [feats[base + idx[s, 2 * jj + i]] for i in range(2)]
                factors[s, jj] = pair_factors(jnp.concatenate(pair, axis=0), recv)

    def second_leg(n, part, size):
        for by in (1, 3):
            for k in range(3):
                send(planes[n][k][0].at[pl.ds(part, size)], planes[n][k][FROM[by]].at[pl.ds(part, size)],
                     w.sem_b2s.at[n, k], w.sem_b2.at[n, k, FROM[by]], line[AXES[k][1]][by])

    def first_leg_done(n):
        for k in range(3):
            wait_for(planes[n][k][0].at[pl.ds(0, 3)], w.sem_b1.at[n, k])

    def lines_second_leg(refs, send_sem, recv_sem):
        for by in STEPS:
            for k in range(3):
                send(refs[k].at[0], refs[k].at[FROM[by]], send_sem.at[k], recv_sem.at[k], line[AXES[k][1]][by])

    @pl.loop(0, SLOTS)
    def _(b):
        feats[2 * NDEV + b] = source_features(w.geo[b])

    build(0, NEAR, 2 * NDEV, 0, 8)
    for k in range(3):
        wait_for(cp[k].at[0, pl.ds(0, 3)], w.sem_c1.at[k])
    lines_second_leg(cp, w.sem_c2s, w.sem_c2)
    second_leg(0, 0, 1)

    w.rem_t[...] = jnp.zeros((2 * NDEV, 8, V), F32)
    w.geo_t[:, 7, :] = jnp.ones((2 * NDEV, V), F32)
    w.en_all[mine] = jnp.zeros((2, V), F32)
    for i in range(3):
        wait_for(w.r1.at[i, pl.ds(0, 7)], w.sem_r.at[i])
    copy = pltpu.make_async_copy(w.r1, w.wanted, w.local_sem)
    copy.start()
    for k in range(3):
        i = DIMS.index(AXES[k][2])
        w.sel[k] = selection(k, jnp.concatenate([w.r1[i, d] for d in range(8)], axis=0))

    build(0, NEAR, 2 * NDEV, 8, 12)
    first_leg_done(0)
    second_leg(0, 1, 1)
    build(0, NEAR, 2 * NDEV, 12, SLOTS)

    def ends(k):
        c = AXES[k][2]
        return [shifted(moved(c, by, o)) for by, o in ((2, 0), (2, 1), (1, 0), (1, 1), (3, 0), (3, 1), (0, 1))]

    def end_index(k, t):
        return t[AXES[k][2]] * 2 + t[1]

    for k in range(3):
        wait_for(cp[k].at[pl.ds(0, 3)], w.sem_c2.at[k])
        for g in range(1 + len(GEO[k])):
            source = cp[k][:, :, g].reshape(256, V)
            got = jnp.dot(w.sel[k], source, preferred_element_type=F32).astype(BF16)
            sg[k][:, g] = got.reshape(8, 32, V)
        me = end_index(k, here)
        rg[k][me] = sg[k][me]
        for to in ends(k):
            send(sg[k].at[end_index(k, to)], rg[k].at[me], w.sem_gs.at[0, k], w.sem_g.at[0, k], to)

    def relay(n):
        for j, by, start in ((1, 3, 0), (3, 1, 2)):
            part = pl.ds(start, 2)
            for k in range(3):
                plane = planes[n][k][j]
                wait_for(plane, w.sem_b2.at[n, k, j])
                send(plane.at[part], planes[n][k][2].at[part],
                     w.sem_b2s.at[n, k], w.sem_b2.at[n, k, 2], line[AXES[k][1]][by])

    def spread(n, j):
        for k in range(3):
            a, b, c = AXES[k]
            wi = DIMS.index(c)
            plane = planes[n][k][j]
            if j == 2:
                wait_for(plane, w.sem_b2.at[n, k, j])
            owners = []
            for i in range(4):
                t = list(here)
                t[a] = (here[a] + i) & 3
                t[b] = (here[b] + j) & 3
                owners.append((t, flat(t)))

            @pl.loop(0, 8)
            def _(d):
                for i, (t, o) in enumerate(owners):
                    for h in range(2):
                        w.ss[k, d, j, t[a], h] = plane[i, w.wanted[wi, d, h, o]]

            me = end_index(k, here)
            for i, (t, o) in enumerate(owners):
                for h in range(2):
                    block = plane[i, w.wanted[wi, me, h, o]]
                    tabs[n][t[0], t[1], t[2], t[3], h, SEG * k : SEG * (k + 1), :] = block
            at = list(owners[0][0])
            at[a] = slice(None)
            goal = tabs[n].at[at[0], at[1], at[2], at[3], :, pl.ds(SEG * k, SEG), :]
            for to in ends(k):
                send(w.ss.at[k, end_index(k, to), j], goal, w.sem_us.at[n, k], w.sem_u.at[n, k], to)

    def applied(load, s, first, count):
        total = None
        for jj in range(first // 2, (first + count) // 2):
            lhs = jnp.concatenate([load(idx[s, 2 * jj + i]) for i in range(2)], axis=1)
            term = jnp.dot(lhs, factors[s, jj], preferred_element_type=F32)
            total = term if total is None else total + term
        return total

    def near_apply():
        @pl.loop(0, SLOTS // 2)
        def _(p):
            for s in (2 * p, 2 * p + 1):
                acc[s] = applied(lambda i: near_s[i], s, 0, NEAR)

    def far_apply(n, start, stop):
        tab = tabs[n]
        r = rows_of((ROWS, V))
        mark = rows_of((2, V)) == n

        def load(i):
            head = tab[i >> 6, (i >> 5) & 1, (i >> 3) & 3, (i >> 1) & 3, i & 1]
            return jnp.concatenate([head, w.tail[i]], axis=0)

        @pl.loop(start // 2, stop // 2)
        def _(p):
            both = [(s, applied(load, s, NEAR, FAR)) for s in (2 * p, 2 * p + 1)]
            for s, far in both:
                a = [alb_ref[i, pl.ds(s, 1), :] for i in range(3)]
                total = (acc[s] + far) * jnp.where(r < 25, a[0], jnp.where(r < 50, a[1], a[2]))
                w.wide[:, s, :] = total
                if n == 0:
                    value = total.astype(BF16)
                    near_s[s] = value
                    for k in range(3):
                        planes[1][k][0][0, s] = value[SEG * k : SEG * (k + 1)]
                energy = jnp.sum(total * total * area_ref[pl.ds(s, 1), :], axis=0, keepdims=True)
                w.en_all[mine] += jnp.where(mark, energy, 0.0)

    def tails(rows_of_part):
        for k in range(3):
            w.rem_t[:, k, :] = jnp.dot(canonical(k), rows_of_part(k), preferred_element_type=F32)
        w.tail[...] = w.rem_t[...].astype(BF16)

    second_leg(0, 2, 2)
    copy.wait()
    spread(0, 0)
    for k in range(3):
        wait_for(rg[k].at[pl.ds(0, 7)], w.sem_g.at[0, k])
        order = canonical(k)
        for g, comp in enumerate(GEO[k]):
            rows = rg[k][:, 1 + g].reshape(256, V)
            w.geo_t[:, comp, :] = jnp.dot(order, rows, preferred_element_type=F32)
    tails(lambda k: rg[k][:, 0].reshape(256, V))

    @pl.loop(0, 2 * NDEV)
    def _(b):
        feats[b] = source_features(w.geo_t[b])

    relay(0)
    spread(0, 1)
    spread(0, 3)
    build(NEAR, FAR, 0, 0, 6)
    spread(0, 2)
    build(NEAR, FAR, 0, 6, SLOTS)
    near_apply()
    for k in range(3):
        wait_for(w.ss.at[k, pl.ds(0, 7)], w.sem_u.at[0, k])

    def half_leg(start):
        part = pl.ds(start, SLOTS // 2)
        for by in STEPS:
            for k in range(3):
                line0 = planes[1][k][0]
                send(line0.at[0, part], line0.at[FROM[by], part],
                     w.sem_b1s.at[1, k], w.sem_b1.at[1, k], line[AXES[k][0]][by])

    far_apply(0, 0, SLOTS // 2)
    half_leg(0)
    far_apply(0, SLOTS // 2, SLOTS)
    for k in range(3):
        w.cr[k, 0, 0] = w.wide[72 + k].astype(BF16)
    cr = [w.cr.at[k] for k in range(3)]
    first_leg([c.at[0] for c in cr], w.sem_r1s, w.sem_r1)
    half_leg(SLOTS // 2)
    second_leg(1, 0, 1)
    b1_ref[...] = w.wide[:CH].astype(BF16)
    for k in range(3):
        wait_for(w.ss.at[k, pl.ds(0, 7)], w.sem_us.at[0, k])
    for k in range(3):
        wait_for(cr[k].at[0, pl.ds(0, 3)], w.sem_r1.at[k])
    lines_second_leg(cr, w.sem_r2s, w.sem_r2)
    first_leg_done(1)
    second_leg(1, 1, 3)
    spread(1, 0)
    near_apply()
    for k in range(3):
        wait_for(cr[k].at[pl.ds(0, 3)], w.sem_r2.at[k])
        got = jnp.dot(w.sel[k], w.cr[k].reshape(256, V), preferred_element_type=F32).astype(BF16)
        w.sr[k] = got.reshape(8, 32, V)
        me = end_index(k, here)
        w.rr[k, me] = w.sr[k, me]
        for to in ends(k):
            send(w.sr.at[k, end_index(k, to)], w.rr.at[k, me], w.sem_gs.at[1, k], w.sem_g.at[1, k], to)
    relay(1)
    for j in (1, 3, 2):
        spread(1, j)
    for k in range(3):
        wait_for(w.rr.at[k, pl.ds(0, 7)], w.sem_g.at[1, k])
    tails(lambda k: w.rr[k].reshape(256, V))
    for k in range(3):
        wait_for(w.ss.at[k, pl.ds(0, 7)], w.sem_u.at[1, k])
    far_apply(1, 0, SLOTS)

    for off in ORDER:
        send(w.en_all.at[mine], w.en_all.at[mine], w.sem_e.at[0], w.sem_e.at[1], shifted(off))
    b2_ref[...] = w.wide[:CH].astype(BF16)
    wait_for(w.en_all.at[pl.ds(0, NDEV - 1)], w.sem_e.at[1])
    en_ref[...] = jnp.sum(w.en_all[...], axis=0)
    wait_for(w.en_all.at[pl.ds(0, NDEV - 1)], w.sem_e.at[0])
    for k in range(3):
        wait_for(w.r1.at[k, pl.ds(0, 7)], w.sem_rs.at[k])
        wait_for(cp[k].at[0, pl.ds(0, 3)], w.sem_c1s.at[k])
        wait_for(cp[k].at[pl.ds(0, 3)], w.sem_c2s.at[k])
        wait_for(cr[k].at[0, pl.ds(0, 3)], w.sem_r1s.at[k])
        wait_for(cr[k].at[pl.ds(0, 3)], w.sem_r2s.at[k])
        wait_for(rg[k].at[pl.ds(0, 7)], w.sem_gs.at[0, k])
        wait_for(w.rr.at[k, pl.ds(0, 7)], w.sem_gs.at[1, k])
        wait_for(w.ss.at[k, pl.ds(0, 7)], w.sem_us.at[1, k])
        for n in range(2):
            wait_for(planes[n][k][0].at[pl.ds(0, 3)], w.sem_b1s.at[n, k])
            for j in (1, 2, 3):
                wait_for(planes[n][k][j], w.sem_b2s.at[n, k])


def last_kernel(b1_ref, b2_ref, en_ref, o1_ref, o2_ref, sum_ref):
    o1_ref[...] = b1_ref[...]
    o2_ref[...] = b2_ref[...]
    for i in range(2):
        sum_ref[i] = jnp.sum(en_ref[i : i + 1, :]) * (1.0 / (NDEV * SLOTS * CH * V))


def scratch_list():
    vm, dma = pltpu.VMEM, pltpu.SemaphoreType.DMA
    out = [
        ("r1", vm((3, 8, 2, V), I32)),
        ("wanted", pltpu.SMEM((3, 8, 2, V), I32)),
        ("near_s", vm((SLOTS, ROWS, V), BF16)),
        ("wide", vm((ROWS, SLOTS, V), F32)),
        ("geo", vm((SLOTS, 8, V), F32)),
        ("sel", vm((3, 256, 256), BF16)),
        ("cr", vm((3, 4, 4, SLOTS, V), BF16)),
        ("sr", vm((3, 8, 32, V), BF16)),
        ("rr", vm((3, 8, 32, V), BF16)),
        ("ss", vm((3, 8, 4, 4, 2, SEG, V), BF16)),
        ("tab_a", vm((4, 2, 4, 4, 2, 3 * SEG, V), BF16)),
        ("tab_b", vm((4, 2, 4, 4, 2, 3 * SEG, V), BF16)),
        ("geo_t", vm((2 * NDEV, 8, V), F32)),
        ("rem_t", vm((2 * NDEV, 8, V), F32)),
        ("tail", vm((2 * NDEV, 8, V), BF16)),
        ("feats", vm((2 * NDEV + SLOTS, 64, V), BF16)),
        ("factors", vm((SLOTS, (NEAR + FAR) // 2, 2 * V, V), BF16)),
        ("acc", vm((SLOTS, ROWS, V), F32)),
        ("en_all", vm((NDEV, 2, V), F32)),
        ("local_sem", dma),
        ("sem_e", dma((2,))),
        ("sem_b2", dma((2, 3, 4))),
    ]
    for k in range(3):
        size = 1 + len(GEO[k])
        out.append((f"cp{k}", vm((4, 4, size, SLOTS, V), BF16)))
        out.append((f"sg{k}", vm((8, size, 32, V), BF16)))
        out.append((f"rg{k}", vm((8, size, 32, V), BF16)))
        for n, j in itertools.product(range(2), range(4)):
            out.append((f"p{n}{k}{j}", vm((4, SLOTS, SEG, V), BF16)))
    for name in ("r", "rs", "c1", "c1s", "c2", "c2s", "r1", "r1s", "r2", "r2s"):
        out.append((f"sem_{name}", dma((3,))))
    for name in ("b1", "b1s", "b2s", "u", "us", "g", "gs"):
        out.append((f"sem_{name}", dma((2, 3))))
    return out


def body(transfer, positions, normals, area, albedo, pairs, home):
    vm = pl.BlockSpec(memory_space=pltpu.VMEM)
    sm = pl.BlockSpec(memory_space=pltpu.SMEM)
    idx, req = pl.pallas_call(
        index_kernel,
        out_shape=(jax.ShapeDtypeStruct((SLOTS, V), I32), jax.ShapeDtypeStruct((2, V), I32)),
        in_specs=[vm, vm],
        out_specs=(vm, vm),
        scratch_shapes=[pltpu.VMEM((SLOTS, V), I32)],
    )(pairs, home.reshape(16, V))
    major = lambda t: jnp.swapaxes(t, 0, 1)
    bounce = jax.ShapeDtypeStruct((CH, SLOTS, V), BF16)
    b1, b2, en = pl.pallas_call(
        main_kernel,
        out_shape=(bounce, bounce, jax.ShapeDtypeStruct((2, V), F32)),
        in_specs=[sm, vm, vm, vm, vm, vm, vm],
        out_specs=(vm, vm, vm),
        scratch_shapes=[shape for _, shape in scratch_list()],
        compiler_params=pltpu.CompilerParams(
            collective_id=0, has_side_effects=True, vmem_limit_bytes=62 * 2**20
        ),
    )(idx, req, major(transfer), major(positions), major(normals), area, major(albedo))
    b1, b2, energies = pl.pallas_call(
        last_kernel,
        out_shape=(bounce, bounce, jax.ShapeDtypeStruct((2,), F32)),
        in_specs=[vm, vm, vm],
        out_specs=(vm, vm, sm),
    )(b1, b2, en)
    return major(b1), major(b2), energies


def solution(mesh):
    finer = Mesh(mesh.devices.reshape(SZ), AX)
    split = [P(AX, *([None] * n)) for n in (2, 2, 2, 1, 2, 1)]
    return jax.shard_map(
        body,
        mesh=finer,
        in_specs=(*split, P()),
        out_specs=(split[0], split[0], P()),
        check_vma=False,
    )
```

```python
import itertools
import types

import jax
import jax.numpy as jnp
import numpy as np
from jax import lax
from jax.experimental import pallas as pl
from jax.experimental.pallas import tpu as pltpu
from jax.sharding import Mesh
from jax.sharding import PartitionSpec as P

AX = ("y", "c", "z", "x")
SZ = (4, 2, 4, 4)
NDEV = 128
SLOTS, NEAR, FAR, CH, V = 16, 16, 24, 75, 128
ROWS = 80
F32, BF16, I32 = jnp.float32, jnp.bfloat16, jnp.int32
MESH = pl.DeviceIdType.MESH


def rounded(t):
    return t.astype(BF16).astype(F32)


def pieces3(t):
    a = rounded(t)
    b = rounded(t - a)
    return a, b, rounded(t - a - b)


def rows_of(shape):
    return lax.broadcasted_iota(I32, shape, 0)


def source_features(v):
    r = rows_of((8, V))
    vh = rounded(v)
    vl = rounded(v - vh)
    m = -(v * v[6:7])
    mh = rounded(m)
    ml = rounded(m - mh)
    x = jnp.where(r < 3, v, 0.0)
    c = pieces3(jnp.sum(pltpu.roll(m, 5, 0) * x, axis=0, keepdims=True))
    e = pieces3(jnp.sum(x * x, axis=0, keepdims=True) + 1.0)
    cv = jnp.ones((8, V), F32)
    for i, row in enumerate(c + e):
        cv = jnp.where(r == i, row, cv)
    return jnp.concatenate([vh, vh, vl, mh, mh, ml, cv, jnp.zeros((8, V), F32)], axis=0).astype(BF16)


def receiver_features(v):
    r = rows_of((8, V))
    z = jnp.zeros((8, V), F32)
    x = jnp.where(r < 3, v, 0.0)
    n = jnp.where(r < 3, pltpu.roll(v, 5, 0), 0.0) * (1.0 / np.pi)
    nh = rounded(n)
    nl = rounded(n - nh)
    xh = rounded(x)
    xl = rounded(x - xh)
    k = pieces3(-jnp.sum(n * x, axis=0, keepdims=True))
    q = pieces3(jnp.sum(x * x, axis=0, keepdims=True))
    xh3 = -pltpu.roll(xh, 3, 0)
    xl3 = -pltpu.roll(xl, 3, 0)
    last = r == 7
    ap = [jnp.where(last, k[0], nh), jnp.where(last, k[1], nl), nh, z, z, z, jnp.where(r == 6, k[2], z), z]
    aq = [z, z, z, xh3, xl3, xh3, jnp.where(r < 3, 1.0, z), z]
    d = [jnp.where(last, q[0], -2.0 * xh), jnp.where(last, q[1], -2.0 * xl), -2.0 * xh, z, z, z,
         jnp.where((r >= 3) & (r < 6), 1.0, jnp.where(r == 6, q[2], z)), z]
    ap, aq, d = (jnp.concatenate(t, axis=0).astype(BF16) for t in (ap, aq, d))
    o = jnp.zeros((64, V), BF16)
    top = jnp.concatenate([ap, aq, o, o, d, o], axis=1)
    bottom = jnp.concatenate([o, o, ap, aq, o, d], axis=1)
    return jnp.concatenate([top, bottom], axis=0)


def pair_factors(feats, recv):
    out = lax.dot_general(feats, recv, (((0,), (0,)), ((), ())), preferred_element_type=F32)
    parts = []
    for i in range(2):
        ap = out[:, 256 * i : 256 * i + 128]
        aq = out[:, 256 * i + 128 : 256 * i + 256]
        d = out[:, 512 + 128 * i : 640 + 128 * i]
        parts.append((jnp.maximum(ap, 0.0) * jnp.maximum(aq, 0.0) / (d * d)).astype(BF16))
    return jnp.concatenate(parts, axis=0)


def me4():
    return tuple(lax.axis_index(a) for a in AX)


def my_index():
    y, c, z, x = me4()
    return ((y * 2 + c) * 4 + z) * 4 + x


def shifted(off):
    return tuple(lax.rem(i + o, s) for i, o, s in zip(me4(), off, SZ))


def flat(t):
    return ((t[0] * 2 + t[1]) * 4 + t[2]) * 4 + t[3]


def index_kernel(pairs_ref, home_ref, idx_ref, req_ref, wide_ref):
    wide_ref[...] = jnp.zeros((SLOTS, V), I32)
    wide_ref[:, : NEAR + FAR] = pairs_ref[...]
    p = wide_ref[...]
    home = home_ref[...]
    shape = (SLOTS, V)
    lane = lax.broadcasted_iota(I32, shape, 1)
    low, high = p & 127, p >> 7
    slot = jnp.zeros(shape, I32)
    for h in range(16):
        got = jnp.take_along_axis(jnp.broadcast_to(home[h : h + 1], shape), low, axis=1)
        slot = jnp.where(high == h, got, slot)
    owner, local = slot >> 4, slot & 15
    lo = jnp.full(shape, 99, I32)
    hi = jnp.full(shape, -1, I32)
    for j in range(NEAR, NEAR + FAR):
        same = owner[:, j : j + 1] == lane
        lo = jnp.where(same, jnp.minimum(lo, local[:, j : j + 1]), lo)
        hi = jnp.where(same, jnp.maximum(hi, local[:, j : j + 1]), hi)
    lo = jnp.min(lo, axis=0, keepdims=True)
    hi = jnp.max(hi, axis=0, keepdims=True)
    lo = jnp.where(lo > 15, 0, lo)
    hi = jnp.where(hi < 0, 0, hi)
    first = jnp.take_along_axis(jnp.broadcast_to(lo, shape), owner, axis=1)
    far = owner * 2 + jnp.where(local != first, 1, 0)
    idx_ref[...] = jnp.where(lane < NEAR, local, far)
    req_ref[...] = jnp.where(rows_of((2, V)) == 0, lo, hi)


OFFSETS = [o for o in itertools.product(range(4), range(2), range(4), range(4)) if any(o)]
ORDER = [OFFSETS[i] for i in np.random.RandomState(0).permutation(len(OFFSETS))]

DIMS = (0, 2, 3)
AXES = ((0, 2, 3), (2, 3, 0), (3, 0, 2))
STEPS = (2, 1, 3)
SEG = 24
GEO = ((0, 1, 2), (3, 4), (5, 6))
FROM = (0, 3, 2, 1)


def moved(dim, by, core=0):
    off = [0, core, 0, 0]
    off[dim] = by
    return tuple(off)


def send(src, dst, send_sem, recv_sem, to):
    pltpu.make_async_remote_copy(
        src, dst, send_sem, recv_sem, device_id=to, device_id_type=MESH
    ).start()


def wait_for(part, sem):
    pltpu.make_async_copy(part, part, sem).wait()


def row_column(shape):
    return rows_of(shape), lax.broadcasted_iota(I32, shape, 1)


def selection(k, table):
    here = me4()
    a, b, _ = AXES[k]
    r, m = row_column((256, 16))
    expand = jnp.where(m == ((r >> 5) << 1) + (r & 1), 1.0, 0.0).astype(BF16)
    wide = jnp.dot(expand, table.astype(F32).astype(BF16), preferred_element_type=F32)
    r, lane = row_column((256, V))
    coords = list(here)
    coords[a] = (here[a] + ((r >> 1) & 3)) & 3
    coords[b] = (here[b] + ((r >> 3) & 3)) & 3
    value = jnp.sum(jnp.where(lane == flat(coords), wide, 0.0), axis=1, keepdims=True)
    r, lane = row_column((256, 256))
    place = (lane - (((r >> 1) & 15) << 4)).astype(F32)
    return jnp.where(value == place, 1.0, 0.0).astype(BF16)


def canonical(k):
    here = me4()
    a, b, c = AXES[k]
    r, col = row_column((256, 256))
    t = (r >> 6, (r >> 5) & 1, (r >> 3) & 3, (r >> 1) & 3)
    i = (t[a] - here[a]) & 3
    j = (t[b] - here[b]) & 3
    place = (((t[c] << 1) + t[1]) << 5) + (j << 3) + (i << 1) + (r & 1)
    return jnp.where(place == col, 1.0, 0.0).astype(BF16)


def main_kernel(idx, req_ref, tr_ref, pos_ref, nrm_ref, area_ref, alb_ref, b1_ref, b2_ref, en_ref, *scratch):
    w = types.SimpleNamespace(**dict(zip([n for n, _ in scratch_list()], scratch)))
    factors, feats, acc, near_s = w.factors, w.feats, w.acc, w.near_s
    cp, sg, rg = (w.cp0, w.cp1, w.cp2), (w.sg0, w.sg1, w.sg2), (w.rg0, w.rg1, w.rg2)
    planes = [[[getattr(w, f"p{n}{k}{j}") for j in range(4)] for k in range(3)] for n in range(2)]
    tabs = (w.tab_a, w.tab_b)
    here = me4()
    core = here[1]
    mine = my_index()
    partner = shifted((0, 1, 0, 0))
    line = {d: {by: shifted(moved(d, by)) for by in STEPS} for d in DIMS}
    other = {d: {by: shifted(moved(d, by, 1)) for by in STEPS} for d in DIMS}

    barrier = pltpu.get_barrier_semaphore()
    greeted = [partner] + [t[d][by] for t in (line, other) for d in DIMS for by in STEPS]
    for to in greeted:
        pl.semaphore_signal(barrier, inc=1, device_id=to, device_id_type=MESH)

    for i in range(3):
        w.r1[i, here[DIMS[i]] * 2 + core] = req_ref[...]
    w.wide[:CH] = tr_ref[...].astype(F32)
    w.wide[CH:] = jnp.zeros((ROWS - CH, SLOTS, V), F32)
    comps = [pos_ref.at[0], pos_ref.at[1], pos_ref.at[2], nrm_ref.at[0], nrm_ref.at[1], nrm_ref.at[2], area_ref]
    for i, comp in enumerate(comps):
        w.geo[:, i, :] = comp[...]
    w.geo[:, 7, :] = jnp.ones((SLOTS, V), F32)
    for s in range(SLOTS):
        value = w.wide[:, s, :].astype(BF16)
        near_s[s] = value
        for k in range(3):
            planes[0][k][0][0, s] = value[SEG * k : SEG * (k + 1)]
    for k in range(3):
        cp[k][0, 0, 0] = tr_ref[72 + k]
        for g, comp in enumerate(GEO[k]):
            cp[k][0, 0, 1 + g] = comps[comp][...].astype(BF16)
    pl.semaphore_wait(barrier, len(greeted))

    for i in range(3):
        slot = w.r1.at[i, here[DIMS[i]] * 2 + core]
        for to in [line[DIMS[i]][by] for by in STEPS] + [other[DIMS[i]][by] for by in STEPS] + [partner]:
            send(req_ref, slot, w.sem_rs.at[i], w.sem_r.at[i], to)

    def first_leg(refs, send_sem, recv_sem):
        for by in STEPS:
            for k in range(3):
                send(refs[k].at[0], refs[k].at[FROM[by]], send_sem.at[k], recv_sem.at[k], line[AXES[k][0]][by])

    first_leg([c.at[0] for c in cp], w.sem_c1s, w.sem_c1)
    first_leg([p[0] for p in planes[0]], w.sem_b1s.at[0], w.sem_b1.at[0])

    def build(first, count, base, start, stop):
        @pl.loop(start, stop)
        def _(s):
            recv = receiver_features(w.geo[s])
            for jj in range(first // 2, (first + count) // 2):
                pair = [feats[base + idx[s, 2 * jj + i]] for i in range(2)]
                factors[s, jj] = pair_factors(jnp.concatenate(pair, axis=0), recv)

    def second_leg(n, part, size):
        for by in (1, 3):
            for k in range(3):
                send(planes[n][k][0].at[pl.ds(part, size)], planes[n][k][FROM[by]].at[pl.ds(part, size)],
                     w.sem_b2s.at[n, k], w.sem_b2.at[n, k, FROM[by]], line[AXES[k][1]][by])

    def first_leg_done(n):
        for k in range(3):
            wait_for(planes[n][k][0].at[pl.ds(0, 3)], w.sem_b1.at[n, k])

    def lines_second_leg(refs, send_sem, recv_sem):
        for by in STEPS:
            for k in range(3):
                send(refs[k].at[0], refs[k].at[FROM[by]], send_sem.at[k], recv_sem.at[k], line[AXES[k][1]][by])

    @pl.loop(0, SLOTS)
    def _(b):
        feats[2 * NDEV + b] = source_features(w.geo[b])

    build(0, NEAR, 2 * NDEV, 0, 8)
    for k in range(3):
        wait_for(cp[k].at[0, pl.ds(0, 3)], w.sem_c1.at[k])
    lines_second_leg(cp, w.sem_c2s, w.sem_c2)
    second_leg(0, 0, 1)

    w.rem_t[...] = jnp.zeros((2 * NDEV, 8, V), F32)
    w.geo_t[:, 7, :] = jnp.ones((2 * NDEV, V), F32)
    w.en_all[mine] = jnp.zeros((2, V), F32)
    for i in range(3):
        wait_for(w.r1.at[i, pl.ds(0, 7)], w.sem_r.at[i])
    copy = pltpu.make_async_copy(w.r1, w.wanted, w.local_sem)
    copy.start()
    for k in range(3):
        i = DIMS.index(AXES[k][2])
        w.sel[k] = selection(k, jnp.concatenate([w.r1[i, d] for d in range(8)], axis=0))

    build(0, NEAR, 2 * NDEV, 8, 12)
    first_leg_done(0)
    second_leg(0, 1, 1)
    build(0, NEAR, 2 * NDEV, 12, SLOTS)

    def ends(k):
        c = AXES[k][2]
        return [shifted(moved(c, by, o)) for by, o in ((2, 0), (2, 1), (1, 0), (1, 1), (3, 0), (3, 1), (0, 1))]

    def end_index(k, t):
        return t[AXES[k][2]] * 2 + t[1]

    for k in range(3):
        wait_for(cp[k].at[pl.ds(0, 3)], w.sem_c2.at[k])
        for g in range(1 + len(GEO[k])):
            source = cp[k][:, :, g].reshape(256, V)
            got = jnp.dot(w.sel[k], source, preferred_element_type=F32).astype(BF16)
            sg[k][:, g] = got.reshape(8, 32, V)
        me = end_index(k, here)
        rg[k][me] = sg[k][me]
        for to in ends(k):
            send(sg[k].at[end_index(k, to)], rg[k].at[me], w.sem_gs.at[0, k], w.sem_g.at[0, k], to)

    def relay(n):
        for j, by, start in ((1, 3, 0), (3, 1, 2)):
            part = pl.ds(start, 2)
            for k in range(3):
                plane = planes[n][k][j]
                wait_for(plane, w.sem_b2.at[n, k, j])
                send(plane.at[part], planes[n][k][2].at[part],
                     w.sem_b2s.at[n, k], w.sem_b2.at[n, k, 2], line[AXES[k][1]][by])

    def spread(n, j):
        for k in range(3):
            a, b, c = AXES[k]
            wi = DIMS.index(c)
            plane = planes[n][k][j]
            if j == 2:
                wait_for(plane, w.sem_b2.at[n, k, j])
            owners = []
            for i in range(4):
                t = list(here)
                t[a] = (here[a] + i) & 3
                t[b] = (here[b] + j) & 3
                owners.append((t, flat(t)))

            @pl.loop(0, 8)
            def _(d):
                for i, (t, o) in enumerate(owners):
                    for h in range(2):
                        w.ss[k, d, j, t[a], h] = plane[i, w.wanted[wi, d, h, o]]

            me = end_index(k, here)
            for i, (t, o) in enumerate(owners):
                for h in range(2):
                    block = plane[i, w.wanted[wi, me, h, o]]
                    tabs[n][t[0], t[1], t[2], t[3], h, SEG * k : SEG * (k + 1), :] = block
            at = list(owners[0][0])
            at[a] = slice(None)
            goal = tabs[n].at[at[0], at[1], at[2], at[3], :, pl.ds(SEG * k, SEG), :]
            for to in ends(k):
                send(w.ss.at[k, end_index(k, to), j], goal, w.sem_us.at[n, k], w.sem_u.at[n, k], to)

    def applied(load, s, first, count):
        total = None
        for jj in range(first // 2, (first + count) // 2):
            lhs = jnp.concatenate([load(idx[s, 2 * jj + i]) for i in range(2)], axis=1)
            term = jnp.dot(lhs, factors[s, jj], preferred_element_type=F32)
            total = term if total is None else total + term
        return total

    def near_apply():
        @pl.loop(0, SLOTS // 2)
        def _(p):
            for s in (2 * p, 2 * p + 1):
                acc[s] = applied(lambda i: near_s[i], s, 0, NEAR)

    def far_apply(n, start, stop):
        tab = tabs[n]
        r = rows_of((ROWS, V))
        mark = rows_of((2, V)) == n

        def load(i):
            head = tab[i >> 6, (i >> 5) & 1, (i >> 3) & 3, (i >> 1) & 3, i & 1]
            return jnp.concatenate([head, w.tail[i]], axis=0)

        @pl.loop(start // 2, stop // 2)
        def _(p):
            both = [(s, applied(load, s, NEAR, FAR)) for s in (2 * p, 2 * p + 1)]
            for s, far in both:
                a = [alb_ref[i, pl.ds(s, 1), :] for i in range(3)]
                total = (acc[s] + far) * jnp.where(r < 25, a[0], jnp.where(r < 50, a[1], a[2]))
                w.wide[:, s, :] = total
                if n == 0:
                    value = total.astype(BF16)
                    near_s[s] = value
                    for k in range(3):
                        planes[1][k][0][0, s] = value[SEG * k : SEG * (k + 1)]
                energy = jnp.sum(total * total * area_ref[pl.ds(s, 1), :], axis=0, keepdims=True)
                w.en_all[mine] += jnp.where(mark, energy, 0.0)

    def tails(rows_of_part):
        for k in range(3):
            w.rem_t[:, k, :] = jnp.dot(canonical(k), rows_of_part(k), preferred_element_type=F32)
        w.tail[...] = w.rem_t[...].astype(BF16)

    second_leg(0, 2, 2)
    copy.wait()
    spread(0, 0)
    near_apply()
    for k in range(3):
        wait_for(rg[k].at[pl.ds(0, 7)], w.sem_g.at[0, k])
        order = canonical(k)
        for g, comp in enumerate(GEO[k]):
            rows = rg[k][:, 1 + g].reshape(256, V)
            w.geo_t[:, comp, :] = jnp.dot(order, rows, preferred_element_type=F32)
    tails(lambda k: rg[k][:, 0].reshape(256, V))

    @pl.loop(0, 2 * NDEV)
    def _(b):
        feats[b] = source_features(w.geo_t[b])

    relay(0)
    spread(0, 1)
    spread(0, 3)
    build(NEAR, FAR, 0, 0, 6)
    spread(0, 2)
    build(NEAR, FAR, 0, 6, SLOTS)
    for k in range(3):
        wait_for(w.ss.at[k, pl.ds(0, 7)], w.sem_u.at[0, k])

    def half_leg(start):
        part = pl.ds(start, SLOTS // 2)
        for by in STEPS:
            for k in range(3):
                line0 = planes[1][k][0]
                send(line0.at[0, part], line0.at[FROM[by], part],
                     w.sem_b1s.at[1, k], w.sem_b1.at[1, k], line[AXES[k][0]][by])

    far_apply(0, 0, SLOTS // 2)
    half_leg(0)
    far_apply(0, SLOTS // 2, SLOTS)
    for k in range(3):
        w.cr[k, 0, 0] = w.wide[72 + k].astype(BF16)
    cr = [w.cr.at[k] for k in range(3)]
    first_leg([c.at[0] for c in cr], w.sem_r1s, w.sem_r1)
    half_leg(SLOTS // 2)
    second_leg(1, 0, 1)
    b1_ref[...] = w.wide[:CH].astype(BF16)
    for k in range(3):
        wait_for(w.ss.at[k, pl.ds(0, 7)], w.sem_us.at[0, k])
    for k in range(3):
        wait_for(cr[k].at[0, pl.ds(0, 3)], w.sem_r1.at[k])
    lines_second_leg(cr, w.sem_r2s, w.sem_r2)
    first_leg_done(1)
    second_leg(1, 1, 3)
    spread(1, 0)
    near_apply()
    for k in range(3):
        wait_for(cr[k].at[pl.ds(0, 3)], w.sem_r2.at[k])
        got = jnp.dot(w.sel[k], w.cr[k].reshape(256, V), preferred_element_type=F32).astype(BF16)
        w.sr[k] = got.reshape(8, 32, V)
        me = end_index(k, here)
        w.rr[k, me] = w.sr[k, me]
        for to in ends(k):
            send(w.sr.at[k, end_index(k, to)], w.rr.at[k, me], w.sem_gs.at[1, k], w.sem_g.at[1, k], to)
    relay(1)
    for j in (1, 3, 2):
        spread(1, j)
    for k in range(3):
        wait_for(w.rr.at[k, pl.ds(0, 7)], w.sem_g.at[1, k])
    tails(lambda k: w.rr[k].reshape(256, V))
    for k in range(3):
        wait_for(w.ss.at[k, pl.ds(0, 7)], w.sem_u.at[1, k])
    far_apply(1, 0, SLOTS)

    for off in ORDER:
        send(w.en_all.at[mine], w.en_all.at[mine], w.sem_e.at[0], w.sem_e.at[1], shifted(off))
    b2_ref[...] = w.wide[:CH].astype(BF16)
    wait_for(w.en_all.at[pl.ds(0, NDEV - 1)], w.sem_e.at[1])
    en_ref[...] = jnp.sum(w.en_all[...], axis=0)
    wait_for(w.en_all.at[pl.ds(0, NDEV - 1)], w.sem_e.at[0])
    for k in range(3):
        wait_for(w.r1.at[k, pl.ds(0, 7)], w.sem_rs.at[k])
        wait_for(cp[k].at[0, pl.ds(0, 3)], w.sem_c1s.at[k])
        wait_for(cp[k].at[pl.ds(0, 3)], w.sem_c2s.at[k])
        wait_for(cr[k].at[0, pl.ds(0, 3)], w.sem_r1s.at[k])
        wait_for(cr[k].at[pl.ds(0, 3)], w.sem_r2s.at[k])
        wait_for(rg[k].at[pl.ds(0, 7)], w.sem_gs.at[0, k])
        wait_for(w.rr.at[k, pl.ds(0, 7)], w.sem_gs.at[1, k])
        wait_for(w.ss.at[k, pl.ds(0, 7)], w.sem_us.at[1, k])
        for n in range(2):
            wait_for(planes[n][k][0].at[pl.ds(0, 3)], w.sem_b1s.at[n, k])
            for j in (1, 2, 3):
                wait_for(planes[n][k][j], w.sem_b2s.at[n, k])


def last_kernel(b1_ref, b2_ref, en_ref, o1_ref, o2_ref, sum_ref):
    o1_ref[...] = b1_ref[...]
    o2_ref[...] = b2_ref[...]
    for i in range(2):
        sum_ref[i] = jnp.sum(en_ref[i : i + 1, :]) * (1.0 / (NDEV * SLOTS * CH * V))


def scratch_list():
    vm, dma = pltpu.VMEM, pltpu.SemaphoreType.DMA
    out = [
        ("r1", vm((3, 8, 2, V), I32)),
        ("wanted", pltpu.SMEM((3, 8, 2, V), I32)),
        ("near_s", vm((SLOTS, ROWS, V), BF16)),
        ("wide", vm((ROWS, SLOTS, V), F32)),
        ("geo", vm((SLOTS, 8, V), F32)),
        ("sel", vm((3, 256, 256), BF16)),
        ("cr", vm((3, 4, 4, SLOTS, V), BF16)),
        ("sr", vm((3, 8, 32, V), BF16)),
        ("rr", vm((3, 8, 32, V), BF16)),
        ("ss", vm((3, 8, 4, 4, 2, SEG, V), BF16)),
        ("tab_a", vm((4, 2, 4, 4, 2, 3 * SEG, V), BF16)),
        ("tab_b", vm((4, 2, 4, 4, 2, 3 * SEG, V), BF16)),
        ("geo_t", vm((2 * NDEV, 8, V), F32)),
        ("rem_t", vm((2 * NDEV, 8, V), F32)),
        ("tail", vm((2 * NDEV, 8, V), BF16)),
        ("feats", vm((2 * NDEV + SLOTS, 64, V), BF16)),
        ("factors", vm((SLOTS, (NEAR + FAR) // 2, 2 * V, V), BF16)),
        ("acc", vm((SLOTS, ROWS, V), F32)),
        ("en_all", vm((NDEV, 2, V), F32)),
        ("local_sem", dma),
        ("sem_e", dma((2,))),
        ("sem_b2", dma((2, 3, 4))),
    ]
    for k in range(3):
        size = 1 + len(GEO[k])
        out.append((f"cp{k}", vm((4, 4, size, SLOTS, V), BF16)))
        out.append((f"sg{k}", vm((8, size, 32, V), BF16)))
        out.append((f"rg{k}", vm((8, size, 32, V), BF16)))
        for n, j in itertools.product(range(2), range(4)):
            out.append((f"p{n}{k}{j}", vm((4, SLOTS, SEG, V), BF16)))
    for name in ("r", "rs", "c1", "c1s", "c2", "c2s", "r1", "r1s", "r2", "r2s"):
        out.append((f"sem_{name}", dma((3,))))
    for name in ("b1", "b1s", "b2s", "u", "us", "g", "gs"):
        out.append((f"sem_{name}", dma((2, 3))))
    return out


def body(transfer, positions, normals, area, albedo, pairs, home):
    vm = pl.BlockSpec(memory_space=pltpu.VMEM)
    sm = pl.BlockSpec(memory_space=pltpu.SMEM)
    idx, req = pl.pallas_call(
        index_kernel,
        out_shape=(jax.ShapeDtypeStruct((SLOTS, V), I32), jax.ShapeDtypeStruct((2, V), I32)),
        in_specs=[vm, vm],
        out_specs=(vm, vm),
        scratch_shapes=[pltpu.VMEM((SLOTS, V), I32)],
    )(pairs, home.reshape(16, V))
    major = lambda t: jnp.swapaxes(t, 0, 1)
    bounce = jax.ShapeDtypeStruct((CH, SLOTS, V), BF16)
    b1, b2, en = pl.pallas_call(
        main_kernel,
        out_shape=(bounce, bounce, jax.ShapeDtypeStruct((2, V), F32)),
        in_specs=[sm, vm, vm, vm, vm, vm, vm],
        out_specs=(vm, vm, vm),
        scratch_shapes=[shape for _, shape in scratch_list()],
        compiler_params=pltpu.CompilerParams(
            collective_id=0, has_side_effects=True, vmem_limit_bytes=62 * 2**20
        ),
    )(idx, req, major(transfer), major(positions), major(normals), area, major(albedo))
    b1, b2, energies = pl.pallas_call(
        last_kernel,
        out_shape=(bounce, bounce, jax.ShapeDtypeStruct((2,), F32)),
        in_specs=[vm, vm, vm],
        out_specs=(vm, vm, sm),
    )(b1, b2, en)
    return major(b1), major(b2), energies


def solution(mesh):
    finer = Mesh(mesh.devices.reshape(SZ), AX)
    split = [P(AX, *([None] * n)) for n in (2, 2, 2, 1, 2, 1)]
    return jax.shard_map(
        body,
        mesh=finer,
        in_specs=(*split, P()),
        out_specs=(split[0], split[0], P()),
        check_vma=False,
    )
```
